32 devices in a mesh: trial: 4 (over y, x), fsdp: 2 (over core), cols: 4 (over z).
Axes of the slice: x: 2, y: 2, z: 4, core: 2. Of those that a mesh axis runs over, the one named last changes fastest.
Arguments:
- train_gate: bfloat16 [8192, 8192], P(('trial', 'fsdp'), 'cols'), parts along dimension 0, may hold values from -0.1875 to 0.1875
- low_gate: bfloat16 [8192, 16], P(('trial', 'fsdp')), parts along dimension 0, may hold values from -0.125 to 0.125
- high_gate: bfloat16 [64, 8192], P('trial', 'cols'), parts along dimension 0, may hold values from -1.5 to 1.5
- train_up: bfloat16 [8192, 8192], P(('trial', 'fsdp'), 'cols'), parts along dimension 0, may hold values from -0.1875 to 0.1875
- low_up: bfloat16 [8192, 16], P(('trial', 'fsdp')), parts along dimension 0, may hold values from -0.125 to 0.125
- high_up: bfloat16 [64, 8192], P('trial', 'cols'), parts along dimension 0, may hold values from -1.5 to 1.5
- norm_gain: float32 [8192], P(('trial', 'fsdp')), parts along dimension 0, may hold values from 0.25 to 1.75
Outputs:
- ready_gate: bfloat16 [8192, 8192], P('trial', 'cols'), parts along dimension 0
- ready_up: bfloat16 [8192, 8192], P('trial', 'cols'), parts along dimension 0
- column_gate: float32 [32768], P(('trial', 'cols')), parts along dimension 0
- column_up: float32 [32768], P(('trial', 'cols')), parts along dimension 0
The draws below stay inside these ranges and needn't reach their ends.
There are 4 independent parts, one for each index of `trial`. The reference program is written for one: setup_inputs(seed, part) draws one part's arguments, and reference() takes and returns one part's arrays. A program takes and returns all parts, laid end to end along the dimension named above; each array names one. Nothing has to cross between parts.
All inputs are finite; a program needn't handle non-finite values. Where the reference program divides by a largest or mean magnitude, that divisor is 1e-20 or more.
Results may differ from the reference program's by a relative error of at most 0.001.
Values may be sent and summed in bfloat16 or wider, within the bound.
No kernel may reach another device: no remote copies, remote signals or barrier semaphores. Data moves between devices by JAX's collectives and lax.ppermute only.
A program may use at most 128 MiB of HBM per device.

```python
import jax
import jax.numpy as jnp

D_MODEL = 2048
D_INNER = 8192
RANK = 16


def spiked(drawn, own_key, source, target, shards_of, factor):
    owner, partner = [(jnp.arange(drawn.shape[axis_at]) // (drawn.shape[axis_at] // shards_of)).reshape([-1 if axis == axis_at else 1 for axis in range(drawn.ndim)]) for axis_at in (source, target)]
    chosen = jax.random.permutation(own_key, shards_of)[partner]
    strong = (owner == chosen) | (owner == (partner + shards_of // 2) % shards_of)
    return jnp.where(strong, factor * drawn, drawn)


def levels(key, shape, split, least, high):
    def one(dim, parts):
        draws = jax.random.uniform(jax.random.fold_in(jax.random.fold_in(key, 6), dim), (parts,), jnp.float32, least / len(split), high / len(split))
        return jnp.repeat(jnp.exp(draws), shape[dim] // parts).reshape((-1,) + (1,) * (len(shape) - dim - 1))

    factor_of = one(*split[0])
    for cut in split[1:]:
        factor_of = factor_of * one(*cut)
    return factor_of


def gaussian(own_key, shape, spread, bound, shards=(), held_as=jnp.bfloat16):
    drawn = jax.random.normal(own_key, shape, jnp.float32) * spread
    if len(shards) > 0:
        drawn = levels(own_key, shape, shards, -0.22, 0.18) * drawn
    return jnp.clip(drawn, min=-bound, max=bound).astype(held_as)


def gaussian_with(stream_key, shape, spread, bound, split, heavy, kind=jnp.bfloat16):
    array = spread * jax.random.normal(stream_key, shape, jnp.float32)
    if split:
        array = array * levels(stream_key, shape, split, -0.22, 0.18)
    return jnp.clip(spiked(array, jax.random.fold_in(stream_key, 3), *heavy), -bound, bound).astype(kind)


def setup_inputs(seed: int = 0, part: int = 0) -> dict:
    seeds = jax.random.split(jax.random.key(seed), 8)
    own_keys = jax.random.split(jax.random.fold_in(seeds[7], part), 8)
    train_gate = gaussian_with(own_keys[0], (D_MODEL, D_INNER), D_MODEL ** -0.5, 0.1875, ((0, 2), (1, 4)), (0, 1, 4, 2.0))
    low_gate = gaussian(own_keys[1], (D_MODEL, RANK), D_MODEL ** -0.5, 0.125, ((0, 2),))
    high_gate = gaussian(own_keys[2], (RANK, D_INNER), RANK ** -0.5, 1.5, ((1, 4),))
    train_up = gaussian_with(own_keys[3], (D_MODEL, D_INNER), D_MODEL ** -0.5, 0.1875, ((0, 2), (1, 4)), (0, 1, 4, 2.0))
    low_up = gaussian(own_keys[4], (D_MODEL, RANK), D_MODEL ** -0.5, 0.125, ((0, 2),))
    high_up = gaussian(own_keys[5], (RANK, D_INNER), RANK ** -0.5, 1.5, ((1, 4),))
    norm_gain = jnp.clip(1.0 + 0.15 * jax.random.normal(own_keys[6], (D_MODEL,), jnp.float32), 0.25, 1.75)
    return {"train_gate": train_gate, "low_gate": low_gate, "high_gate": high_gate, "train_up": train_up, "low_up": low_up, "high_up": high_up, "norm_gain": norm_gain}


mix_rate = 1.0


def reference(train_gate, low_gate, high_gate, train_up, low_up, high_up, norm_gain):
    latest_gate = train_gate.astype(jnp.float32) + mix_rate * jnp.dot(low_gate, high_gate, preferred_element_type=jnp.float32)
    latest_up = train_up.astype(jnp.float32) + mix_rate * jnp.dot(low_up, high_up, preferred_element_type=jnp.float32)
    latest_gained_gate = latest_gate * norm_gain[:, None]
    latest_gained_up = latest_up * norm_gain[:, None]
    column_gate = jnp.max(jnp.abs(latest_gained_gate), axis=0)
    ready_gate = (latest_gained_gate / column_gate).astype(jnp.bfloat16)
    column_up = jnp.max(jnp.abs(latest_gained_up), axis=0)
    ready_up = (latest_gained_up / column_up).astype(jnp.bfloat16)
    return ready_gate, ready_up, column_gate, column_up
```

```python
import functools

import jax
import jax.numpy as jnp
from jax import lax
from jax.experimental import pallas as pl
from jax.experimental.pallas import tpu as pltpu
from jax.sharding import PartitionSpec as P

mix_rate = 1.0
LANES = 128
SUBLANES = 8
TILE = 256
HBM = pl.BlockSpec(memory_space=pl.ANY)
VMEM = pl.BlockSpec(memory_space=pltpu.VMEM)
f32, bf16 = jnp.float32, jnp.bfloat16


def in_hbm(x):
    return pltpu.with_memory_space_constraint(x, pltpu.HBM)


def in_vmem(x):
    return pltpu.with_memory_space_constraint(x, pltpu.VMEM)


def spread_gain(gain_row, wide_ref):
    for k in range(wide_ref.shape[0] // LANES):
        row = gain_row(k)
        wide_ref[pl.ds(k * LANES, LANES), :] = jnp.broadcast_to(row, (LANES, LANES)).T


def delta(low, high):
    return mix_rate * jnp.dot(low, high, preferred_element_type=f32)


def columns_of(j):
    return pl.ds(pl.multiple_of(j * TILE, TILE), TILE)


def first_kernel(
    pieces,
    train_gate, low_gate, high_gate, train_up, low_up, high_up, gain,
    kept_gate, kept_up, small, *rest,
):
    ups = rest[: len(pieces)]
    (held, low_in, high_in, gain_in, low, wide, peak, sems, small_sems) = rest[len(pieces) :]
    rows, cols = train_gate.shape
    rank = low_gate.shape[0]
    small_copies = [
        pltpu.make_async_copy(src, dst, small_sems.at[n])
        for n, (src, dst) in enumerate(
            (
                (gain, gain_in),
                (low_gate, low_in.at[0]),
                (high_gate, high_in.at[0]),
                (low_up, low_in.at[1]),
                (high_up, high_in.at[1]),
            )
        )
    ]
    starts = [sum(pieces[:k]) for k in range(len(pieces))]
    work = []
    chunk = TILE
    for k in range(rows // chunk):
        at = pl.ds(k * chunk, chunk)
        work.append((0, k * chunk, chunk, train_gate.at[at], held.at[at], kept_gate))
    for k, size in enumerate(pieces):
        work.append((1, starts[k], size, train_up.at[pl.ds(starts[k], size)], ups[k], kept_up))
    copies = [
        pltpu.make_async_copy(src, dst, sems.at[n])
        for n, (_, _, _, src, dst, _) in enumerate(work)
    ]
    for c in small_copies[:3]:
        c.start()
    copies[0].start()
    for c in small_copies[3:]:
        c.start()
    for c in copies[1:]:
        c.start()
    for c in small_copies:
        c.wait()
    spread_gain(lambda k: gain_in[pl.ds(k, 1), :], wide)
    for which in range(2):
        turned = low_in[which].astype(f32)
        small[pl.ds(which * rank, rank), :] = turned
        low[which] = turned.T.astype(bf16)
    for k in range(rows // LANES):
        small[pl.ds(2 * rank, 1), pl.ds(k * LANES, LANES)] = gain_in[pl.ds(k, 1), :]
    peak[...] = jnp.zeros_like(peak)
    for n, (which, start, size, _, src, kept) in enumerate(work):
        copies[n].wait()
        for step in range(size // TILE):
            at = pl.ds(start + step * TILE, TILE)
            from_at = pl.ds(step * TILE, TILE)

            @pl.loop(0, cols // TILE)
            def _(j):
                c = columns_of(j)
                grown = src[from_at, c].astype(f32) + delta(low[which, at, :], high_in[which, :, c])
                gains = wide[at, :]
                gained = grown * jnp.concatenate([gains] * (TILE // LANES), axis=1)
                kept[at, c] = gained
                top = jnp.max(jnp.abs(gained).reshape(TILE // SUBLANES, SUBLANES, TILE), axis=0)
                peak[which, :, c] = jnp.maximum(peak[which, :, c], top)

    line = cols // 2
    for which in range(2):
        top = jnp.max(peak[which], axis=0, keepdims=True)
        for half in range(2):
            small[pl.ds(2 * rank + 1 + 2 * which + half, 1), :] = top[:, half * line : (half + 1) * line]


def top_row(ref, rank, which):
    base = 2 * rank + 1 + 2 * which
    return jnp.concatenate([ref[pl.ds(base, 1), :], ref[pl.ds(base + 1, 1), :]], axis=1)


def my_place(axis):
    return lax.axis_index(axis)


def second_kernel(
    slots,
    kept_gate, kept_up, small, far_small, far_gate, high_gate,
    ready_gate, ready_up, column_gate, column_up, far_low, far_wide, scale,
    out, high, sems, high_sem,
):
    rows, cols = kept_gate.shape
    rank = high_gate.shape[0]
    high_copy = pltpu.make_async_copy(high_gate, high, high_sem)
    high_copy.start()
    me = lax.axis_index("fsdp")
    mine, theirs = me * rows, (1 - me) * rows
    for which, column in ((0, column_gate), (1, column_up)):
        top = jnp.maximum(top_row(small, rank, which), top_row(far_small, rank, which))
        scale[pl.ds(which, 1), :] = 1.0 / top
        for k in range(cols // LANES):
            column[pl.ds(k, 1), :] = top[:, k * LANES : (k + 1) * LANES]
    spread_gain(
        lambda k: far_small[pl.ds(2 * rank, 1), pl.ds(k * LANES, LANES)], far_wide
    )
    for which in range(2):
        far_low[which] = far_small[pl.ds(which * rank, rank), :].T.astype(bf16)
    work = []
    for kept, ready, which in ((kept_gate, ready_gate, 0), (kept_up, ready_up, 1)):
        for k in range(rows // TILE):
            work.append((kept, ready, which, k * TILE, mine))
    for k in range(rows // TILE):
        work.append((None, ready_gate, 0, k * TILE, theirs))
    copies = []
    for n, (kept, ready, which, start, base) in enumerate(work):
        slot = n % slots
        if n >= slots:
            copies[n - slots].wait()
        if n == 2 * (rows // TILE):
            high_copy.wait()
        at = pl.ds(start, TILE)

        @pl.loop(0, cols // TILE)
        def _(j):
            c = columns_of(j)
            factor = jnp.broadcast_to(scale[pl.ds(which, 1), c], (TILE, TILE))
            if kept is not None:
                value = kept[at, c]
            else:
                grown = far_gate[at, c].astype(f32) + delta(far_low[0, at, :], high[:, c])
                value = grown * jnp.concatenate([far_wide[at, :]] * (TILE // LANES), axis=1)
            out[slot, :, c] = (value * factor).astype(bf16)

        to = pl.ds(pl.multiple_of(base + start, TILE), TILE)
        copies.append(pltpu.make_async_copy(out.at[slot], ready.at[to], sems.at[slot]))
        copies[-1].start()
    for c in copies[-slots:]:
        c.wait()


def last_kernel(
    start, far_up, far_low, far_wide, scale, high_up, before, ready_up,
    out, high, sems, high_sem,
):
    size, cols = far_up.shape
    rows = far_wide.shape[0]
    high_copy = pltpu.make_async_copy(high_up, high, high_sem)
    high_copy.start()
    me = lax.axis_index("fsdp")
    theirs = (1 - me) * rows
    high_copy.wait()
    copies = []
    for k in range(size // TILE):
        at = pl.ds(start + k * TILE, TILE)

        @pl.loop(0, cols // TILE)
        def _(j):
            c = columns_of(j)
            factor = jnp.broadcast_to(scale[pl.ds(1, 1), c], (TILE, TILE))
            grown = far_up[pl.ds(k * TILE, TILE), c].astype(f32) + delta(far_low[1, at, :], high[:, c])
            value = grown * jnp.concatenate([far_wide[at, :]] * (TILE // LANES), axis=1)
            out[pl.ds(k * TILE, TILE), c] = (value * factor).astype(bf16)

        to = pl.ds(pl.multiple_of(theirs + start + k * TILE, TILE), TILE)
        copies.append(
            pltpu.make_async_copy(out.at[pl.ds(k * TILE, TILE)], ready_up.at[to], sems.at[k])
        )
        copies[-1].start()
    for c in copies:
        c.wait()


def paired(train_gate, low_gate, high_gate, train_up, low_up, high_up, norm_gain):
    rows, cols = train_gate.shape
    rank = high_gate.shape[0]
    swap = [(0, 1), (1, 0)]
    other = lambda x: lax.ppermute(x, "fsdp", swap)
    pieces = (rows // 2, rows // 4, rows // 4)
    far_gate = other(train_gate)
    n_small = -(-(2 * rank + 5) // SUBLANES) * SUBLANES
    kept = pltpu.VMEM((rows, cols), f32)
    kept_gate, kept_up, small, *ups = pl.pallas_call(
        functools.partial(first_kernel, pieces),
        out_shape=[kept, kept, pltpu.VMEM((n_small, rows), f32)]
        + [pltpu.VMEM((size, cols), bf16) for size in pieces],
        in_specs=[HBM] * 7,
        out_specs=[VMEM] * (3 + len(pieces)),
        scratch_shapes=[
            pltpu.VMEM((rows, cols), bf16),
            pltpu.VMEM((2, rank, rows), bf16),
            pltpu.VMEM((2, rank, cols), bf16),
            pltpu.VMEM((rows // LANES, LANES), f32),
            pltpu.VMEM((2, rows, rank), bf16),
            pltpu.VMEM((rows, LANES), f32),
            pltpu.VMEM((2, SUBLANES, cols), f32),
            pltpu.SemaphoreType.DMA((rows // TILE + len(pieces),)),
            pltpu.SemaphoreType.DMA((5,)),
        ],
        compiler_params=pltpu.CompilerParams(vmem_limit_bytes=8 << 20),
        name="own_half",
    )(
        in_hbm(train_gate), in_hbm(low_gate.T), in_hbm(high_gate),
        in_hbm(train_up), in_hbm(low_up.T), in_hbm(high_up),
        in_hbm(norm_gain.reshape(rows // LANES, LANES)),
    )
    far_small = other(small)
    far_ups = [other(up) for up in ups]
    whole = jax.ShapeDtypeStruct((2 * rows, cols), bf16)
    column = jax.ShapeDtypeStruct((cols // LANES, LANES), f32)
    slots = 6
    ready_gate, ready_up, column_gate, column_up, far_low, far_wide, scale = pl.pallas_call(
        functools.partial(second_kernel, slots),
        out_shape=[
            whole, whole, column, column,
            pltpu.VMEM((2, rows, rank), bf16), pltpu.VMEM((rows, LANES), f32), pltpu.VMEM((2, cols), f32),
        ],
        in_specs=[VMEM] * 5 + [HBM],
        out_specs=[HBM, HBM] + [VMEM] * 5,
        scratch_shapes=[
            pltpu.VMEM((slots, TILE, cols), bf16),
            pltpu.VMEM((rank, cols), bf16),
            pltpu.SemaphoreType.DMA((slots,)),
            pltpu.SemaphoreType.DMA,
        ],
        compiler_params=pltpu.CompilerParams(vmem_limit_bytes=10 << 20),
        name="own_out",
    )(
        in_vmem(kept_gate), in_vmem(kept_up), in_vmem(small), in_vmem(far_small), in_vmem(far_gate),
        in_hbm(high_gate),
    )
    start = 0
    for size, far_up in zip(pieces, far_ups):
        ready_up = pl.pallas_call(
            functools.partial(last_kernel, start),
            out_shape=whole,
            in_specs=[VMEM] * 4 + [HBM, HBM],
            out_specs=HBM,
            scratch_shapes=[
                pltpu.VMEM((size, cols), bf16),
                pltpu.VMEM((rank, cols), bf16),
                pltpu.SemaphoreType.DMA((size // TILE,)),
                pltpu.SemaphoreType.DMA,
            ],
            input_output_aliases={5: 0},
            compiler_params=pltpu.CompilerParams(vmem_limit_bytes=6 << 20),
            name=f"far_up_{start}",
        )(in_vmem(far_up), in_vmem(far_low), in_vmem(far_wide), in_vmem(scale), in_hbm(high_up), ready_up)
        start += size
    return ready_gate, ready_up, column_gate.reshape(cols), column_up.reshape(cols)


def gathered(train_gate, low_gate, high_gate, train_up, low_up, high_up, norm_gain):
    def gained(train, low, high):
        return (train.astype(f32) + delta(low, high)) * norm_gain[:, None]

    gate, up = gained(train_gate, low_gate, high_gate), gained(train_up, low_up, high_up)
    column_gate, column_up = lax.pmax(
        (jnp.max(jnp.abs(gate), axis=0), jnp.max(jnp.abs(up), axis=0)), "fsdp"
    )
    ready_gate, ready_up = (
        lax.all_gather((full / column).astype(bf16), "fsdp", axis=0, tiled=True)
        for full, column in ((gate, column_gate), (up, column_up))
    )
    return ready_gate, ready_up, column_gate, column_up


def solution(mesh):
    placed = (
        P(("trial", "fsdp"), "cols"),
        P(("trial", "fsdp"), None),
        P("trial", "cols"),
        P(("trial", "fsdp"), "cols"),
        P(("trial", "fsdp"), None),
        P("trial", "cols"),
        P(("trial", "fsdp")),
    )
    return jax.shard_map(
        paired if mesh.shape["fsdp"] == 2 else gathered,
        mesh=mesh,
        in_specs=placed,
        out_specs=(
            P("trial", "cols"),
            P("trial", "cols"),
            P(("trial", "cols")),
            P(("trial", "cols")),
        ),
        check_vma=False,
    )
```

```python
import functools

import jax
import jax.numpy as jnp
from jax import lax
from jax.experimental import pallas as pl
from jax.experimental.pallas import tpu as pltpu
from jax.sharding import PartitionSpec as P


mix_rate = 1.0
LANES = 128
SUBLANES = 8
TILE = 256
HBM = pl.BlockSpec(memory_space=pl.ANY)
VMEM = pl.BlockSpec(memory_space=pltpu.VMEM)
f32, bf16 = jnp.float32, jnp.bfloat16


def in_hbm(x):
    return pltpu.with_memory_space_constraint(x, pltpu.HBM)


def in_vmem(x):
    return pltpu.with_memory_space_constraint(x, pltpu.VMEM)


def spread_gain(gain_row, wide_ref):
    for k in range(wide_ref.shape[0] // LANES):
        row = gain_row(k)
        wide_ref[pl.ds(k * LANES, LANES), :] = jnp.broadcast_to(row, (LANES, LANES)).T


def delta(low, high):
    return mix_rate * jnp.dot(low, high, preferred_element_type=f32)


def tiles(cols):
    return [pl.ds(j * TILE, TILE) for j in range(cols // TILE)]


def widened(ref, at):
    return jnp.concatenate([ref[at, :]] * (TILE // LANES), axis=1)


def first_kernel(
    pieces,
    train_gate, low_gate, high_gate, train_up, low_up, high_up, gain,
    kept_gate, kept_up, small, high, *rest,
):
    ups = rest[: len(pieces)]
    (held, low_in, gain_in, low, wide, peak, sems, small_sems) = rest[len(pieces) :]
    rows, cols = train_gate.shape
    rank = low_gate.shape[0]
    small_copies = [
        pltpu.make_async_copy(src, dst, small_sems.at[n])
        for n, (src, dst) in enumerate(
            (
                (gain, gain_in),
                (low_gate, low_in.at[0]),
                (high_gate, high.at[0]),
                (low_up, low_in.at[1]),
                (high_up, high.at[1]),
            )
        )
    ]
    starts = [sum(pieces[:k]) for k in range(len(pieces))]
    work = []
    chunk = TILE
    for k in range(rows // chunk):
        at = pl.ds(k * chunk, chunk)
        work.append((0, k * chunk, chunk, train_gate.at[at], held.at[at], kept_gate))
    for k, size in enumerate(pieces):
        work.append((1, starts[k], size, train_up.at[pl.ds(starts[k], size)], ups[k], kept_up))
    copies = [
        pltpu.make_async_copy(src, dst, sems.at[n])
        for n, (_, _, _, src, dst, _) in enumerate(work)
    ]
    for c in small_copies[:3]:
        c.start()
    copies[0].start()
    for c in small_copies[3:]:
        c.start()
    for c in copies[1:]:
        c.start()
    for c in small_copies:
        c.wait()
    spread_gain(lambda k: gain_in[pl.ds(k, 1), :], wide)
    for which in range(2):
        turned = low_in[which].astype(f32)
        small[pl.ds(which * rank, rank), :] = turned
        low[which] = turned.T.astype(bf16)
    for k in range(rows // LANES):
        small[pl.ds(2 * rank, 1), pl.ds(k * LANES, LANES)] = gain_in[pl.ds(k, 1), :]
    peak[...] = jnp.zeros_like(peak)
    for n, (which, start, size, _, src, kept) in enumerate(work):
        copies[n].wait()
        for step in range(size // TILE):
            at = pl.ds(start + step * TILE, TILE)
            from_at = pl.ds(step * TILE, TILE)

            for c in tiles(cols):
                grown = src[from_at, c].astype(f32) + delta(low[which, at, :], high[which, :, c])
                gained = grown * widened(wide, at)
                kept[at, c] = gained
                top = jnp.max(jnp.abs(gained).reshape(TILE // SUBLANES, SUBLANES, TILE), axis=0)
                peak[which, :, c] = jnp.maximum(peak[which, :, c], top)

    line = cols // 2
    for which in range(2):
        top = jnp.max(peak[which], axis=0, keepdims=True)
        for half in range(2):
            small[pl.ds(2 * rank + 1 + 2 * which + half, 1), :] = top[:, half * line : (half + 1) * line]


def top_row(ref, rank, which):
    base = 2 * rank + 1 + 2 * which
    return jnp.concatenate([ref[pl.ds(base, 1), :], ref[pl.ds(base + 1, 1), :]], axis=1)


def second_kernel(
    slots,
    kept_gate, kept_up, small, far_small, far_gate, high,
    ready_gate, ready_up, column_gate, column_up, far_low, far_wide, scale,
    out, sems,
):
    rows, cols = kept_gate.shape
    rank = high.shape[1]
    me = lax.axis_index("fsdp")
    mine, theirs = me * rows, (1 - me) * rows
    for which, column in ((0, column_gate), (1, column_up)):
        top = jnp.maximum(top_row(small, rank, which), top_row(far_small, rank, which))
        scale[pl.ds(which, 1), :] = 1.0 / top
        for k in range(cols // LANES):
            column[pl.ds(k, 1), :] = top[:, k * LANES : (k + 1) * LANES]
    spread_gain(
        lambda k: far_small[pl.ds(2 * rank, 1), pl.ds(k * LANES, LANES)], far_wide
    )
    for which in range(2):
        far_low[which] = far_small[pl.ds(which * rank, rank), :].T.astype(bf16)
    work = []
    for kept, ready, which in ((kept_gate, ready_gate, 0), (kept_up, ready_up, 1)):
        for k in range(rows // TILE):
            work.append((kept, ready, which, k * TILE, mine))
    for k in range(rows // TILE):
        work.append((None, ready_gate, 0, k * TILE, theirs))
    copies = []
    for n, (kept, ready, which, start, base) in enumerate(work):
        slot = n % slots
        if n >= slots:
            copies[n - slots].wait()
        at = pl.ds(start, TILE)

        for c in tiles(cols):
            factor = jnp.broadcast_to(scale[pl.ds(which, 1), c], (TILE, TILE))
            if kept is not None:
                value = kept[at, c]
            else:
                grown = far_gate[at, c].astype(f32) + delta(far_low[0, at, :], high[0, :, c])
                value = grown * widened(far_wide, at)
            out[slot, :, c] = (value * factor).astype(bf16)

        to = pl.ds(pl.multiple_of(base + start, TILE), TILE)
        copies.append(pltpu.make_async_copy(out.at[slot], ready.at[to], sems.at[slot]))
        copies[-1].start()
    for c in copies[-slots:]:
        c.wait()


def last_kernel(
    start, far_up, far_low, far_wide, scale, high, before, ready_up,
    out, sems,
):
    size, cols = far_up.shape
    rows = far_wide.shape[0]
    me = lax.axis_index("fsdp")
    theirs = (1 - me) * rows
    copies = []
    for k in range(size // TILE):
        at = pl.ds(start + k * TILE, TILE)

        for c in tiles(cols):
            factor = jnp.broadcast_to(scale[pl.ds(1, 1), c], (TILE, TILE))
            grown = far_up[pl.ds(k * TILE, TILE), c].astype(f32) + delta(far_low[1, at, :], high[1, :, c])
            value = grown * widened(far_wide, at)
            out[pl.ds(k * TILE, TILE), c] = (value * factor).astype(bf16)

        to = pl.ds(pl.multiple_of(theirs + start + k * TILE, TILE), TILE)
        copies.append(
            pltpu.make_async_copy(out.at[pl.ds(k * TILE, TILE)], ready_up.at[to], sems.at[k])
        )
        copies[-1].start()
    for c in copies:
        c.wait()


def paired(train_gate, low_gate, high_gate, train_up, low_up, high_up, norm_gain):
    rows, cols = train_gate.shape
    rank = high_gate.shape[0]
    swap = [(0, 1), (1, 0)]
    other = lambda x: lax.ppermute(x, "fsdp", swap)
    pieces = (rows // 2, rows // 4, rows // 4)
    far_gate = other(train_gate)
    n_small = -(-(2 * rank + 5) // SUBLANES) * SUBLANES
    kept = pltpu.VMEM((rows, cols), f32)
    kept_gate, kept_up, small, high, *ups = pl.pallas_call(
        functools.partial(first_kernel, pieces),
        out_shape=[kept, kept, pltpu.VMEM((n_small, rows), f32), pltpu.VMEM((2, rank, cols), bf16)]
        + [pltpu.VMEM((size, cols), bf16) for size in pieces],
        in_specs=[HBM] * 7,
        out_specs=[VMEM] * (4 + len(pieces)),
        scratch_shapes=[
            pltpu.VMEM((rows, cols), bf16),
            pltpu.VMEM((2, rank, rows), bf16),
            pltpu.VMEM((rows // LANES, LANES), f32),
            pltpu.VMEM((2, rows, rank), bf16),
            pltpu.VMEM((rows, LANES), f32),
            pltpu.VMEM((2, SUBLANES, cols), f32),
            pltpu.SemaphoreType.DMA((rows // TILE + len(pieces),)),
            pltpu.SemaphoreType.DMA((5,)),
        ],
        compiler_params=pltpu.CompilerParams(vmem_limit_bytes=8 << 20),
        name="own_half",
    )(
        in_hbm(train_gate), in_hbm(low_gate.T), in_hbm(high_gate),
        in_hbm(train_up), in_hbm(low_up.T), in_hbm(high_up),
        in_hbm(norm_gain.reshape(rows // LANES, LANES)),
    )
    far_small = other(small)
    far_ups = [other(up) for up in ups]
    whole = jax.ShapeDtypeStruct((2 * rows, cols), bf16)
    column = jax.ShapeDtypeStruct((cols // LANES, LANES), f32)
    slots = 6
    ready_gate, ready_up, column_gate, column_up, far_low, far_wide, scale = pl.pallas_call(
        functools.partial(second_kernel, slots),
        out_shape=[
            whole, whole, column, column,
            pltpu.VMEM((2, rows, rank), bf16), pltpu.VMEM((rows, LANES), f32), pltpu.VMEM((2, cols), f32),
        ],
        in_specs=[VMEM] * 6,
        out_specs=[HBM, HBM] + [VMEM] * 5,
        scratch_shapes=[
            pltpu.VMEM((slots, TILE, cols), bf16),
            pltpu.SemaphoreType.DMA((slots,)),
        ],
        compiler_params=pltpu.CompilerParams(vmem_limit_bytes=10 << 20),
        name="own_out",
    )(
        in_vmem(kept_gate), in_vmem(kept_up), in_vmem(small), in_vmem(far_small), in_vmem(far_gate),
        in_vmem(high),
    )
    start = 0
    for size, far_up in zip(pieces, far_ups):
        ready_up = pl.pallas_call(
            functools.partial(last_kernel, start),
            out_shape=whole,
            in_specs=[VMEM] * 5 + [HBM],
            out_specs=HBM,
            scratch_shapes=[
                pltpu.VMEM((size, cols), bf16),
                pltpu.SemaphoreType.DMA((size // TILE,)),
            ],
            input_output_aliases={5: 0},
            compiler_params=pltpu.CompilerParams(vmem_limit_bytes=6 << 20),
        )(in_vmem(far_up), in_vmem(far_low), in_vmem(far_wide), in_vmem(scale), in_vmem(high), ready_up)
        start += size
    return ready_gate, ready_up, column_gate.reshape(cols), column_up.reshape(cols)


def gathered(train_gate, low_gate, high_gate, train_up, low_up, high_up, norm_gain):
    def gained(train, low, high):
        return (train.astype(f32) + delta(low, high)) * norm_gain[:, None]

    gate, up = gained(train_gate, low_gate, high_gate), gained(train_up, low_up, high_up)
    column_gate, column_up = lax.pmax(
        (jnp.max(jnp.abs(gate), axis=0), jnp.max(jnp.abs(up), axis=0)), "fsdp"
    )
    ready_gate, ready_up = (
        lax.all_gather((full / column).astype(bf16), "fsdp", axis=0, tiled=True)
        for full, column in ((gate, column_gate), (up, column_up))
    )
    return ready_gate, ready_up, column_gate, column_up


def solution(mesh):
    placed = (
        P(("trial", "fsdp"), "cols"),
        P(("trial", "fsdp"), None),
        P("trial", "cols"),
        P(("trial", "fsdp"), "cols"),
        P(("trial", "fsdp"), None),
        P("trial", "cols"),
        P(("trial", "fsdp")),
    )
    pair = mesh.shape["fsdp"] == 2
    return jax.shard_map(
        paired if pair else gathered,
        mesh=mesh,
        in_specs=placed,
        out_specs=(
            P("trial", "cols"),
            P("trial", "cols"),
            P(("trial", "cols")),
            P(("trial", "cols")),
        ),
        check_vma=False,
    )
```

```python
import functools

import jax
import jax.numpy as jnp
from jax import lax
from jax.experimental import pallas as pl
from jax.experimental.pallas import tpu as pltpu
from jax.sharding import PartitionSpec as P


mix_rate = 1.0
LANES = 128
SUBLANES = 8
TILE = 256
IN_ROWS = 256
IN_FLIGHT = 3
OWN_ROWS = 128
FAR_ROWS = 256
LAST_ROWS = 128
PARTS = (3, 1)
HBM = pl.BlockSpec(memory_space=pl.ANY)
VMEM = pl.BlockSpec(memory_space=pltpu.VMEM)
f32, bf16 = jnp.float32, jnp.bfloat16


def in_hbm(x):
    return pltpu.with_memory_space_constraint(x, pltpu.HBM)


def in_vmem(x):
    return pltpu.with_memory_space_constraint(x, pltpu.VMEM)


def spread_gain(gain_row, wide_ref):
    for k in range(wide_ref.shape[0] // LANES):
        row = gain_row(k)
        wide_ref[pl.ds(k * LANES, LANES), :] = jnp.broadcast_to(row, (LANES, LANES)).T


def delta(low, high):
    return mix_rate * jnp.dot(low, high, preferred_element_type=f32)


def tiles(cols):
    return [pl.ds(j * TILE, TILE) for j in range(cols // TILE)]


def widened(ref, at):
    return jnp.concatenate([ref[at, :]] * (TILE // LANES), axis=1)


def first_kernel(
    pieces,
    train_gate, low_gate, high_gate, train_up, low_up, high_up, gain,
    kept_gate, kept_up, small, high, *rest,
):
    ups = rest[: len(pieces)]
    held, low_in, gain_in, low, wide, peak, sems, small_sems = rest[len(pieces) :]
    rows, cols = train_gate.shape
    rank = low_gate.shape[0]
    small_copies = [
        pltpu.make_async_copy(src, dst, small_sems.at[n])
        for n, (src, dst) in enumerate(
            (
                (gain, gain_in),
                (low_gate, low_in.at[0]),
                (high_gate, high.at[0]),
                (low_up, low_in.at[1]),
                (high_up, high.at[1]),
            )
        )
    ]
    groups = [(0, 0, rows, train_gate, held, kept_gate)]
    groups += [(1, start, size, train_up, up, kept_up) for up, (start, size) in zip(ups, spans(pieces, rows))]
    copies = []
    for _, start, size, train, dst, _ in groups:
        for at in range(0, size, IN_ROWS):
            n = len(copies)
            copies.append(
                pltpu.make_async_copy(
                    train.at[pl.ds(start + at, IN_ROWS)], dst.at[pl.ds(at, IN_ROWS)], sems.at[n]
                )
            )
    copies[0].start()
    for c in small_copies:
        c.start()
    for c in copies[1:IN_FLIGHT]:
        c.start()
    for c in small_copies:
        c.wait()
    spread_gain(lambda k: gain_in[pl.ds(k, 1), :], wide)
    for which in range(2):
        turned = low_in[which].astype(f32)
        small[pl.ds(which * rank, rank), :] = turned
        low[which] = turned.T.astype(bf16)
    for k in range(rows // LANES):
        small[pl.ds(2 * rank, 1), pl.ds(k * LANES, LANES)] = gain_in[pl.ds(k, 1), :]
    peak[...] = jnp.zeros_like(peak)
    done = 0
    for which, start, size, train, src, kept in groups:
        steps = size // IN_ROWS

        @pl.loop(0, steps)
        def _(k):
            pltpu.make_async_copy(
                train.at[pl.ds(0, IN_ROWS)], src.at[pl.ds(0, IN_ROWS)], sems.at[done + k]
            ).wait()
            for ahead in range(done + IN_FLIGHT, min(done + steps + IN_FLIGHT, len(copies))):
                pl.when(done + k + IN_FLIGHT == ahead)(copies[ahead].start)
            here = pl.ds(pl.multiple_of(k * IN_ROWS, IN_ROWS), IN_ROWS)
            at = pl.ds(pl.multiple_of(start + k * IN_ROWS, IN_ROWS), IN_ROWS)
            for c in tiles(cols):
                grown = src[here, c].astype(f32) + delta(low[which, at, :], high[which, :, c])
                gained = grown * widened(wide, at)
                kept[at, c] = gained
                top = jnp.max(jnp.abs(gained).reshape(IN_ROWS // SUBLANES, SUBLANES, TILE), axis=0)
                peak[which, :, c] = jnp.maximum(peak[which, :, c], top)

        done += steps
    line = cols // 2
    for which in range(2):
        top = jnp.max(peak[which], axis=0, keepdims=True)
        for half in range(2):
            small[pl.ds(2 * rank + 1 + 2 * which + half, 1), :] = top[:, half * line : (half + 1) * line]


def spans(sizes, total):
    start, out = 0, []
    while start < total:
        size = min(sizes[min(len(out), len(sizes) - 1)], total - start)
        out.append((start, size))
        start += size
    return out


def top_row(ref, rank, which):
    base = 2 * rank + 1 + 2 * which
    return jnp.concatenate([ref[pl.ds(base, 1), :], ref[pl.ds(base + 1, 1), :]], axis=1)


def rows_at(base, start, size):
    return pl.ds(pl.multiple_of(base + start, LANES), size)


def scale_far(far, which, start, step, far_low, far_wide, scale, high, out, target, theirs, sems, keep):
    size, cols = far.shape
    steps = size // step

    def copy(k):
        here = pl.ds(pl.multiple_of(k * step, step), step)
        return pltpu.make_async_copy(
            out.at[here], target.at[rows_at(theirs, start + k * step, step)], sems.at[k]
        )

    @pl.loop(0, steps)
    def _(k):
        here = pl.ds(pl.multiple_of(k * step, step), step)
        at = pl.ds(pl.multiple_of(start + k * step, step), step)
        for c in tiles(cols):
            factor = jnp.broadcast_to(scale[pl.ds(which, 1), c], (step, TILE))
            grown = far[here, c].astype(f32) + delta(far_low[which, at, :], high[which, :, c])
            out[here, c] = (grown * widened(far_wide, at) * factor).astype(bf16)
        if keep:
            pl.when(k < steps - keep)(copy(k).start)
        else:
            copy(k).start()

    return [copy(k) for k in range(steps - keep)]


def second_kernel(
    keep,
    kept_gate, kept_up, small, far_small, far_gate, high,
    ready_gate, ready_up, column_gate, column_up, far_low, far_wide, scale, out_far,
    out_gate, out_up, sems, far_sems,
):
    rows, cols = kept_gate.shape
    rank = high.shape[1]
    me = lax.axis_index("fsdp")
    mine, theirs = me * rows, (1 - me) * rows
    waits = []
    for which, kept, ready, out, column in (
        (0, kept_gate, ready_gate, out_gate, column_gate),
        (1, kept_up, ready_up, out_up, column_up),
    ):
        top = jnp.maximum(top_row(small, rank, which), top_row(far_small, rank, which))
        scale[pl.ds(which, 1), :] = 1.0 / top

        def copy(k):
            return pltpu.make_async_copy(
                out.at[pl.ds(pl.multiple_of(k * OWN_ROWS, OWN_ROWS), OWN_ROWS)],
                ready.at[rows_at(mine, k * OWN_ROWS, OWN_ROWS)],
                sems.at[which, k],
            )

        @pl.loop(0, rows // OWN_ROWS)
        def _(k):
            at = pl.ds(pl.multiple_of(k * OWN_ROWS, OWN_ROWS), OWN_ROWS)
            for c in tiles(cols):
                factor = jnp.broadcast_to(scale[pl.ds(which, 1), c], (OWN_ROWS, TILE))
                out[at, c] = (kept[at, c] * factor).astype(bf16)
            copy(k).start()

        waits += [copy(k) for k in range(rows // OWN_ROWS)]
        for k in range(cols // LANES):
            column[pl.ds(k, 1), :] = top[:, k * LANES : (k + 1) * LANES]
    spread_gain(
        lambda k: far_small[pl.ds(2 * rank, 1), pl.ds(k * LANES, LANES)], far_wide
    )
    for w in range(2):
        far_low[w] = far_small[pl.ds(w * rank, rank), :].T.astype(bf16)
    waits += scale_far(
        far_gate, 0, 0, FAR_ROWS, far_low, far_wide, scale, high, out_far, ready_gate, theirs, far_sems, keep
    )
    for c in waits:
        c.wait()


def far_kernel(
    start, step, behind, keep,
    far_up, far_low, far_wide, scale, high, carried, before_gate, before_up,
    ready_gate, ready_up, *rest,
):
    out, sems = rest[:2]
    rows = far_wide.shape[0]
    theirs = (1 - lax.axis_index("fsdp")) * rows
    which, at, size = behind
    n = carried.shape[0]
    carry = pltpu.make_async_copy(
        carried.at[pl.ds(n - size, size)],
        (ready_gate, ready_up)[which].at[rows_at(theirs, at, size)],
        rest[2],
    )
    carry.start()
    waits = scale_far(
        far_up, 1, start, step, far_low, far_wide, scale, high, out, ready_up, theirs, sems, keep
    )
    carry.wait()
    for c in waits:
        c.wait()


def paired(train_gate, low_gate, high_gate, train_up, low_up, high_up, norm_gain):
    rows, cols = train_gate.shape
    rank = high_gate.shape[0]
    swap = [(0, 1), (1, 0)]
    other = lambda x: lax.ppermute(x, "fsdp", swap)
    pieces = tuple(rows * part // sum(PARTS) for part in PARTS)
    far_gate = other(train_gate)
    n_small = -(-(2 * rank + 5) // SUBLANES) * SUBLANES
    kept = pltpu.VMEM((rows, cols), f32)
    kept_gate, kept_up, small, high, *ups = pl.pallas_call(
        functools.partial(first_kernel, pieces),
        out_shape=[kept, kept, pltpu.VMEM((n_small, rows), f32), pltpu.VMEM((2, rank, cols), bf16)]
        + [pltpu.VMEM((size, cols), bf16) for size in pieces],
        in_specs=[HBM] * 7,
        out_specs=[VMEM] * (4 + len(pieces)),
        scratch_shapes=[
            pltpu.VMEM((rows, cols), bf16),
            pltpu.VMEM((2, rank, rows), bf16),
            pltpu.VMEM((rows // LANES, LANES), f32),
            pltpu.VMEM((2, rows, rank), bf16),
            pltpu.VMEM((rows, LANES), f32),
            pltpu.VMEM((2, SUBLANES, cols), f32),
            pltpu.SemaphoreType.DMA((2 * rows // IN_ROWS,)),
            pltpu.SemaphoreType.DMA((5,)),
        ],
        compiler_params=pltpu.CompilerParams(vmem_limit_bytes=8 << 20),
        name="own_half",
    )(
        in_hbm(train_gate), in_hbm(low_gate.T), in_hbm(high_gate),
        in_hbm(train_up), in_hbm(low_up.T), in_hbm(high_up),
        in_hbm(norm_gain.reshape(rows // LANES, LANES)),
    )
    far_small = other(small)
    far_ups = [other(up) for up in ups]
    whole = jax.ShapeDtypeStruct((2 * rows, cols), bf16)
    column = jax.ShapeDtypeStruct((cols // LANES, LANES), f32)
    keep = 1
    ready_gate, ready_up, column_gate, column_up, far_low, far_wide, scale, carry = pl.pallas_call(
        functools.partial(second_kernel, keep),
        out_shape=[
            whole, whole, column, column,
            pltpu.VMEM((2, rows, rank), bf16), pltpu.VMEM((rows, LANES), f32), pltpu.VMEM((2, cols), f32),
            pltpu.VMEM((rows, cols), bf16),
        ],
        in_specs=[VMEM] * 6,
        out_specs=[HBM, HBM] + [VMEM] * 6,
        scratch_shapes=[
            pltpu.VMEM((rows, cols), bf16),
            pltpu.VMEM((rows, cols), bf16),
            pltpu.SemaphoreType.DMA((2, rows // OWN_ROWS)),
            pltpu.SemaphoreType.DMA((rows // FAR_ROWS,)),
        ],
        compiler_params=pltpu.CompilerParams(vmem_limit_bytes=10 << 20),
        name="own_out",
    )(
        in_vmem(kept_gate), in_vmem(kept_up), in_vmem(small), in_vmem(far_small), in_vmem(far_gate),
        in_vmem(high),
    )
    behind = (0, rows - keep * FAR_ROWS, keep * FAR_ROWS)
    for n, ((start, size), far_up) in enumerate(zip(spans(pieces, rows), far_ups)):
        end = n == len(pieces) - 1
        step = LAST_ROWS if end else FAR_ROWS
        keep = 0 if end else 1
        ready_gate, ready_up, *left = pl.pallas_call(
            functools.partial(far_kernel, start, step, behind, keep),
            out_shape=[whole, whole] + [pltpu.VMEM((size, cols), bf16)] * keep,
            in_specs=[VMEM] * 6 + [HBM, HBM],
            out_specs=[HBM, HBM] + [VMEM] * keep,
            scratch_shapes=[pltpu.VMEM((size, cols), bf16)] * (1 - keep)
            + [pltpu.SemaphoreType.DMA((size // step,)), pltpu.SemaphoreType.DMA],
            input_output_aliases={6: 0, 7: 1},
            compiler_params=pltpu.CompilerParams(vmem_limit_bytes=6 << 20),
        )(
            in_vmem(far_up), in_vmem(far_low), in_vmem(far_wide), in_vmem(scale), in_vmem(high),
            in_vmem(carry), ready_gate, ready_up,
        )
        behind = (1, start + size - keep * step, keep * step)
        carry = left[0] if left else None
    return ready_gate, ready_up, column_gate.reshape(cols), column_up.reshape(cols)


def gathered(train_gate, low_gate, high_gate, train_up, low_up, high_up, norm_gain):
    def gained(train, low, high):
        return (train.astype(f32) + delta(low, high)) * norm_gain[:, None]

    gate, up = gained(train_gate, low_gate, high_gate), gained(train_up, low_up, high_up)
    column_gate, column_up = lax.pmax(
        (jnp.max(jnp.abs(gate), axis=0), jnp.max(jnp.abs(up), axis=0)), "fsdp"
    )
    ready_gate, ready_up = (
        lax.all_gather((full / column).astype(bf16), "fsdp", axis=0, tiled=True)
        for full, column in ((gate, column_gate), (up, column_up))
    )
    return ready_gate, ready_up, column_gate, column_up


def solution(mesh):
    placed = (
        P(("trial", "fsdp"), "cols"),
        P(("trial", "fsdp"), None),
        P("trial", "cols"),
        P(("trial", "fsdp"), "cols"),
        P(("trial", "fsdp"), None),
        P("trial", "cols"),
        P(("trial", "fsdp")),
    )
    pair = mesh.shape["fsdp"] == 2
    return jax.shard_map(
        paired if pair else gathered,
        mesh=mesh,
        in_specs=placed,
        out_specs=(
            P("trial", "cols"),
            P("trial", "cols"),
            P(("trial", "cols")),
            P(("trial", "cols")),
        ),
        check_vma=False,
    )
```

```python
import functools

import jax
import jax.numpy as jnp
from jax import lax
from jax.experimental import pallas as pl
from jax.experimental.pallas import tpu as pltpu
from jax.sharding import PartitionSpec as P


mix_rate = 1.0
LANES = 128
SUBLANES = 8
TILE = 256
IN_ROWS = 256
IN_FLIGHT = 3
OWN_ROWS = 128
FAR_ROWS = 256
LAST_ROWS = 128
PARTS = (3, 1)
KEEP = 2
KEEP_UP = 1
HBM = pl.BlockSpec(memory_space=pl.ANY)
VMEM = pl.BlockSpec(memory_space=pltpu.VMEM)
f32, bf16 = jnp.float32, jnp.bfloat16


def in_hbm(x):
    return pltpu.with_memory_space_constraint(x, pltpu.HBM)


def in_vmem(x):
    return pltpu.with_memory_space_constraint(x, pltpu.VMEM)


def spread_gain(gain_row, wide_ref):
    for k in range(wide_ref.shape[0] // LANES):
        row = gain_row(k)
        wide_ref[pl.ds(k * LANES, LANES), :] = jnp.broadcast_to(row, (LANES, LANES)).T


def delta(low, high):
    return mix_rate * jnp.dot(low, high, preferred_element_type=f32)


def tiles(cols):
    return [pl.ds(j * TILE, TILE) for j in range(cols // TILE)]


def widened(ref, at):
    return jnp.concatenate([ref[at, :]] * (TILE // LANES), axis=1)


def first_kernel(
    pieces,
    train_gate, low_gate, high_gate, train_up, low_up, high_up, gain,
    kept_gate, kept_up, small, high, *rest,
):
    ups = rest[: len(pieces)]
    held, low_in, gain_in, low, wide, peak, sems, small_sems = rest[len(pieces) :]
    rows, cols = train_gate.shape
    rank = low_gate.shape[0]
    small_copies = [
        pltpu.make_async_copy(src, dst, small_sems.at[n])
        for n, (src, dst) in enumerate(
            (
                (gain, gain_in),
                (low_gate, low_in.at[0]),
                (high_gate, high.at[0]),
                (low_up, low_in.at[1]),
                (high_up, high.at[1]),
            )
        )
    ]
    groups = [(0, 0, rows, train_gate, held, kept_gate)]
    groups += [(1, start, size, train_up, up, kept_up) for up, (start, size) in zip(ups, spans(pieces, rows))]
    copies = []
    for _, start, size, train, dst, _ in groups:
        for at in range(0, size, IN_ROWS):
            n = len(copies)
            copies.append(
                pltpu.make_async_copy(
                    train.at[pl.ds(start + at, IN_ROWS)], dst.at[pl.ds(at, IN_ROWS)], sems.at[n]
                )
            )
    copies[0].start()
    for c in small_copies:
        c.start()
    for c in copies[1:IN_FLIGHT]:
        c.start()
    for c in small_copies:
        c.wait()
    spread_gain(lambda k: gain_in[pl.ds(k, 1), :], wide)
    for which in range(2):
        turned = low_in[which].astype(f32)
        small[pl.ds(which * rank, rank), :] = turned
        low[which] = turned.T.astype(bf16)
    for k in range(rows // LANES):
        small[pl.ds(2 * rank, 1), pl.ds(k * LANES, LANES)] = gain_in[pl.ds(k, 1), :]
    peak[...] = jnp.zeros_like(peak)
    done = 0
    for which, start, size, train, src, kept in groups:
        steps = size // IN_ROWS

        @pl.loop(0, steps)
        def _(k):
            pltpu.make_async_copy(
                train.at[pl.ds(0, IN_ROWS)], src.at[pl.ds(0, IN_ROWS)], sems.at[done + k]
            ).wait()
            for ahead in range(done + IN_FLIGHT, min(done + steps + IN_FLIGHT, len(copies))):
                pl.when(done + k + IN_FLIGHT == ahead)(copies[ahead].start)
            here = pl.ds(pl.multiple_of(k * IN_ROWS, IN_ROWS), IN_ROWS)
            at = pl.ds(pl.multiple_of(start + k * IN_ROWS, IN_ROWS), IN_ROWS)
            for c in tiles(cols):
                grown = src[here, c].astype(f32) + delta(low[which, at, :], high[which, :, c])
                gained = grown * widened(wide, at)
                kept[at, c] = gained
                top = jnp.max(jnp.abs(gained).reshape(IN_ROWS // SUBLANES, SUBLANES, TILE), axis=0)
                peak[which, :, c] = jnp.maximum(peak[which, :, c], top)

        done += steps
    line = cols // 2
    for which in range(2):
        top = jnp.max(peak[which], axis=0, keepdims=True)
        for half in range(2):
            small[pl.ds(2 * rank + 1 + 2 * which + half, 1), :] = top[:, half * line : (half + 1) * line]


def spans(sizes, total):
    start, out = 0, []
    while start < total:
        size = min(sizes[min(len(out), len(sizes) - 1)], total - start)
        out.append((start, size))
        start += size
    return out


def top_row(ref, rank, which):
    base = 2 * rank + 1 + 2 * which
    return jnp.concatenate([ref[pl.ds(base, 1), :], ref[pl.ds(base + 1, 1), :]], axis=1)


def rows_at(base, start, size):
    return pl.ds(pl.multiple_of(base + start, LANES), size)


def scale_far(far, which, start, step, far_low, far_wide, scale, high, out, target, theirs, sems, keep):
    size, cols = far.shape
    steps = size // step

    def copy(k):
        here = pl.ds(pl.multiple_of(k * step, step), step)
        return pltpu.make_async_copy(
            out.at[here], target.at[rows_at(theirs, start + k * step, step)], sems.at[k]
        )

    @pl.loop(0, steps)
    def _(k):
        here = pl.ds(pl.multiple_of(k * step, step), step)
        at = pl.ds(pl.multiple_of(start + k * step, step), step)
        for c in tiles(cols):
            factor = jnp.broadcast_to(scale[pl.ds(which, 1), c], (step, TILE))
            grown = far[here, c].astype(f32) + delta(far_low[which, at, :], high[which, :, c])
            out[here, c] = (grown * widened(far_wide, at) * factor).astype(bf16)
        if keep:
            pl.when(k < steps - keep)(copy(k).start)
        else:
            copy(k).start()

    return [copy(k) for k in range(steps - keep)]


def second_kernel(
    keep,
    kept_gate, kept_up, small, far_small, far_gate, high,
    ready_gate, ready_up, column_gate, column_up, far_low, far_wide, scale, out_far,
    out_gate, out_up, column, sems, far_sems, column_sems,
):
    rows, cols = kept_gate.shape
    rank = high.shape[1]
    me = lax.axis_index("fsdp")
    mine, theirs = me * rows, (1 - me) * rows
    waits = []
    for which, kept, ready, out, column_to in (
        (0, kept_gate, ready_gate, out_gate, column_gate),
        (1, kept_up, ready_up, out_up, column_up),
    ):
        top = jnp.maximum(top_row(small, rank, which), top_row(far_small, rank, which))
        scale[pl.ds(which, 1), :] = 1.0 / top

        def copy(k):
            return pltpu.make_async_copy(
                out.at[pl.ds(pl.multiple_of(k * OWN_ROWS, OWN_ROWS), OWN_ROWS)],
                ready.at[rows_at(mine, k * OWN_ROWS, OWN_ROWS)],
                sems.at[which, k],
            )

        @pl.loop(0, rows // OWN_ROWS)
        def _(k):
            at = pl.ds(pl.multiple_of(k * OWN_ROWS, OWN_ROWS), OWN_ROWS)
            for c in tiles(cols):
                factor = jnp.broadcast_to(scale[pl.ds(which, 1), c], (OWN_ROWS, TILE))
                out[at, c] = (kept[at, c] * factor).astype(bf16)
            copy(k).start()

        waits += [copy(k) for k in range(rows // OWN_ROWS)]
        for k in range(cols // LANES):
            column[which, pl.ds(k, 1), :] = top[:, k * LANES : (k + 1) * LANES]
        waits.append(pltpu.make_async_copy(column.at[which], column_to, column_sems.at[which]))
        waits[-1].start()
    spread_gain(
        lambda k: far_small[pl.ds(2 * rank, 1), pl.ds(k * LANES, LANES)], far_wide
    )
    for w in range(2):
        far_low[w] = far_small[pl.ds(w * rank, rank), :].T.astype(bf16)
    waits += scale_far(
        far_gate, 0, 0, FAR_ROWS, far_low, far_wide, scale, high, out_far, ready_gate, theirs, far_sems, keep
    )
    for c in waits:
        c.wait()


def far_kernel(
    start, step, behind, keep,
    far_up, far_low, far_wide, scale, high, carried, before_gate, before_up,
    ready_gate, ready_up, *rest,
):
    out, sems = rest[:2]
    rows = far_wide.shape[0]
    theirs = (1 - lax.axis_index("fsdp")) * rows
    which, at, size = behind
    n = carried.shape[0]
    carry = pltpu.make_async_copy(
        carried.at[pl.ds(n - size, size)],
        (ready_gate, ready_up)[which].at[rows_at(theirs, at, size)],
        rest[2],
    )
    carry.start()
    waits = scale_far(
        far_up, 1, start, step, far_low, far_wide, scale, high, out, ready_up, theirs, sems, keep
    )
    carry.wait()
    for c in waits:
        c.wait()


def paired(train_gate, low_gate, high_gate, train_up, low_up, high_up, norm_gain):
    rows, cols = train_gate.shape
    rank = high_gate.shape[0]
    swap = [(0, 1), (1, 0)]
    other = lambda x: lax.ppermute(x, "fsdp", swap)
    pieces = tuple(rows * part // sum(PARTS) for part in PARTS)
    far_gate = other(train_gate)
    n_small = -(-(2 * rank + 5) // SUBLANES) * SUBLANES
    kept = pltpu.VMEM((rows, cols), f32)
    kept_gate, kept_up, small, high, *ups = pl.pallas_call(
        functools.partial(first_kernel, pieces),
        out_shape=[kept, kept, pltpu.VMEM((n_small, rows), f32), pltpu.VMEM((2, rank, cols), bf16)]
        + [pltpu.VMEM((size, cols), bf16) for size in pieces],
        in_specs=[HBM] * 7,
        out_specs=[VMEM] * (4 + len(pieces)),
        scratch_shapes=[
            pltpu.VMEM((rows, cols), bf16),
            pltpu.VMEM((2, rank, rows), bf16),
            pltpu.VMEM((rows // LANES, LANES), f32),
            pltpu.VMEM((2, rows, rank), bf16),
            pltpu.VMEM((rows, LANES), f32),
            pltpu.VMEM((2, SUBLANES, cols), f32),
            pltpu.SemaphoreType.DMA((2 * rows // IN_ROWS,)),
            pltpu.SemaphoreType.DMA((5,)),
        ],
        compiler_params=pltpu.CompilerParams(vmem_limit_bytes=8 << 20),
        name="own_half",
    )(
        in_hbm(train_gate), in_hbm(low_gate.T), in_hbm(high_gate),
        in_hbm(train_up), in_hbm(low_up.T), in_hbm(high_up),
        in_hbm(norm_gain.reshape(rows // LANES, LANES)),
    )
    far_small = other(small)
    far_ups = [other(up) for up in ups]
    whole = jax.ShapeDtypeStruct((2 * rows, cols), bf16)
    column = jax.ShapeDtypeStruct((cols // LANES, LANES), f32)
    keep = KEEP
    ready_gate, ready_up, column_gate, column_up, far_low, far_wide, scale, carry = pl.pallas_call(
        functools.partial(second_kernel, keep),
        out_shape=[
            whole, whole, column, column,
            pltpu.VMEM((2, rows, rank), bf16), pltpu.VMEM((rows, LANES), f32), pltpu.VMEM((2, cols), f32),
            pltpu.VMEM((rows, cols), bf16),
        ],
        in_specs=[VMEM] * 6,
        out_specs=[HBM] * 4 + [VMEM] * 4,
        scratch_shapes=[
            pltpu.VMEM((rows, cols), bf16),
            pltpu.VMEM((rows, cols), bf16),
            pltpu.VMEM((2, cols // LANES, LANES), f32),
            pltpu.SemaphoreType.DMA((2, rows // OWN_ROWS)),
            pltpu.SemaphoreType.DMA((rows // FAR_ROWS,)),
            pltpu.SemaphoreType.DMA((2,)),
        ],
        compiler_params=pltpu.CompilerParams(vmem_limit_bytes=10 << 20),
        name="own_out",
    )(
        in_vmem(kept_gate), in_vmem(kept_up), in_vmem(small), in_vmem(far_small), in_vmem(far_gate),
        in_vmem(high),
    )
    behind = (0, rows - keep * FAR_ROWS, keep * FAR_ROWS)
    for n, ((start, size), far_up) in enumerate(zip(spans(pieces, rows), far_ups)):
        end = n == len(pieces) - 1
        step = LAST_ROWS if end else FAR_ROWS
        keep = 0 if end else KEEP_UP
        ready_gate, ready_up, *left = pl.pallas_call(
            functools.partial(far_kernel, start, step, behind, keep),
            out_shape=[whole, whole] + [pltpu.VMEM((size, cols), bf16)] * (keep > 0),
            in_specs=[VMEM] * 6 + [HBM, HBM],
            out_specs=[HBM, HBM] + [VMEM] * (keep > 0),
            scratch_shapes=[pltpu.VMEM((size, cols), bf16)] * (keep == 0)
            + [pltpu.SemaphoreType.DMA((size // step,)), pltpu.SemaphoreType.DMA],
            input_output_aliases={6: 0, 7: 1},
            compiler_params=pltpu.CompilerParams(vmem_limit_bytes=6 << 20),
        )(
            in_vmem(far_up), in_vmem(far_low), in_vmem(far_wide), in_vmem(scale), in_vmem(high),
            in_vmem(carry), ready_gate, ready_up,
        )
        behind = (1, start + size - keep * step, keep * step)
        carry = left[0] if left else None
    return ready_gate, ready_up, column_gate.reshape(cols), column_up.reshape(cols)


def gathered(train_gate, low_gate, high_gate, train_up, low_up, high_up, norm_gain):
    def gained(train, low, high):
        return (train.astype(f32) + delta(low, high)) * norm_gain[:, None]

    gate, up = gained(train_gate, low_gate, high_gate), gained(train_up, low_up, high_up)
    column_gate, column_up = lax.pmax(
        (jnp.max(jnp.abs(gate), axis=0), jnp.max(jnp.abs(up), axis=0)), "fsdp"
    )
    ready_gate, ready_up = (
        lax.all_gather((full / column).astype(bf16), "fsdp", axis=0, tiled=True)
        for full, column in ((gate, column_gate), (up, column_up))
    )
    return ready_gate, ready_up, column_gate, column_up


def solution(mesh):
    placed = (
        P(("trial", "fsdp"), "cols"),
        P(("trial", "fsdp"), None),
        P("trial", "cols"),
        P(("trial", "fsdp"), "cols"),
        P(("trial", "fsdp"), None),
        P("trial", "cols"),
        P(("trial", "fsdp")),
    )
    pair = mesh.shape["fsdp"] == 2
    return jax.shard_map(
        paired if pair else gathered,
        mesh=mesh,
        in_specs=placed,
        out_specs=(
            P("trial", "cols"),
            P("trial", "cols"),
            P(("trial", "cols")),
            P(("trial", "cols")),
        ),
        check_vma=False,
    )
```

```python
import functools

import jax
import jax.numpy as jnp
from jax import lax
from jax.experimental import pallas as pl
from jax.experimental.pallas import tpu as pltpu
from jax.sharding import PartitionSpec as P


mix_rate = 1.0
LANES = 128
SUBLANES = 8
TILE = 256
GATE_STEPS = 4
UP_STEPS = (2, 2)
IN_FLIGHT = 3
OWN_ROWS = 128
FAR_ROWS = 256
HEAD_ROWS = 128
LAST_ROWS = 128
PARTS = (5, 3)
KEEP = 2
AHEAD_ROWS = 192
KEEP_UP = 3
HBM = pl.BlockSpec(memory_space=pl.ANY)
VMEM = pl.BlockSpec(memory_space=pltpu.VMEM)
f32, bf16 = jnp.float32, jnp.bfloat16


def in_hbm(x):
    return pltpu.with_memory_space_constraint(x, pltpu.HBM)


def in_vmem(x):
    return pltpu.with_memory_space_constraint(x, pltpu.VMEM)


def spread_gain(gain_row, wide_ref):
    for k in range(wide_ref.shape[0] // LANES):
        row = gain_row(k)
        wide_ref[pl.ds(k * LANES, LANES), :] = jnp.broadcast_to(row, (LANES, LANES)).T


def delta(low, high):
    return mix_rate * jnp.dot(low, high, preferred_element_type=f32)


def tiles(cols):
    return [pl.ds(j * TILE, TILE) for j in range(cols // TILE)]


def widened(ref, at):
    return jnp.concatenate([ref[at, :]] * (TILE // LANES), axis=1)


def first_kernel(
    pieces,
    train_gate, low_gate, high_gate, train_up, low_up, high_up, gain,
    kept_gate, kept_up, small, high, *rest,
):
    ups = rest[: len(pieces)]
    held, low_in, gain_in, low, wide, peak, sems, small_sems = rest[len(pieces) :]
    rows, cols = train_gate.shape
    rank = low_gate.shape[0]
    small_copies = [
        pltpu.make_async_copy(src, dst, small_sems.at[n])
        for n, (src, dst) in enumerate(
            (
                (gain, gain_in),
                (low_gate, low_in.at[0]),
                (high_gate, high.at[0]),
                (low_up, low_in.at[1]),
                (high_up, high.at[1]),
            )
        )
    ]
    groups = [(0, 0, rows, rows // GATE_STEPS, train_gate, held, kept_gate)]
    groups += [
        (1, start, size, size // steps, train_up, up, kept_up)
        for up, (start, size), steps in zip(ups, spans(pieces, rows), UP_STEPS)
    ]
    copies = []
    for _, start, size, step, train, dst, _ in groups:
        for at in range(0, size, step):
            n = len(copies)
            copies.append(
                pltpu.make_async_copy(
                    train.at[pl.ds(start + at, step)], dst.at[pl.ds(at, step)], sems.at[n]
                )
            )
    copies[0].start()
    for c in small_copies:
        c.start()
    for c in copies[1:IN_FLIGHT]:
        c.start()
    for c in small_copies:
        c.wait()
    spread_gain(lambda k: gain_in[pl.ds(k, 1), :], wide)
    for which in range(2):
        turned = low_in[which].astype(f32)
        small[pl.ds(which * rank, rank), :] = turned
        low[which] = turned.T.astype(bf16)
    for k in range(rows // LANES):
        small[pl.ds(2 * rank, 1), pl.ds(k * LANES, LANES)] = gain_in[pl.ds(k, 1), :]
    peak[...] = jnp.zeros_like(peak)
    done = 0
    for which, start, size, step, train, src, kept in groups:
        steps = size // step

        @pl.loop(0, steps)
        def _(k):
            pltpu.make_async_copy(
                train.at[pl.ds(0, step)], src.at[pl.ds(0, step)], sems.at[done + k]
            ).wait()
            for ahead in range(done + IN_FLIGHT, min(done + steps + IN_FLIGHT, len(copies))):
                pl.when(done + k + IN_FLIGHT == ahead)(copies[ahead].start)
            here = pl.ds(pl.multiple_of(k * step, step), step)
            at = pl.ds(pl.multiple_of(start + k * step, 64), step)
            for c in tiles(cols):
                grown = src[here, c].astype(f32) + delta(low[which, at, :], high[which, :, c])
                gained = grown * widened(wide, at)
                kept[at, c] = gained
                top = jnp.max(jnp.abs(gained).reshape(step // SUBLANES, SUBLANES, TILE), axis=0)
                peak[which, :, c] = jnp.maximum(peak[which, :, c], top)

        done += steps
    line = cols // 2
    for which in range(2):
        top = jnp.max(peak[which], axis=0, keepdims=True)
        for half in range(2):
            small[pl.ds(2 * rank + 1 + 2 * which + half, 1), :] = top[:, half * line : (half + 1) * line]


def spans(sizes, total):
    start, out = 0, []
    while start < total:
        size = min(sizes[min(len(out), len(sizes) - 1)], total - start)
        out.append((start, size))
        start += size
    return out


def top_row(ref, rank, which):
    base = 2 * rank + 1 + 2 * which
    return jnp.concatenate([ref[pl.ds(base, 1), :], ref[pl.ds(base + 1, 1), :]], axis=1)


def rows_at(base, start, size):
    return pl.ds(pl.multiple_of(base + start, 64), size)


def scale_far(far, which, start, step, far_low, far_wide, scale, high, out, target, theirs, sems, keep):
    size, cols = far.shape
    steps = size // step

    def copy(k):
        here = pl.ds(pl.multiple_of(k * step, step), step)
        return pltpu.make_async_copy(
            out.at[here], target.at[rows_at(theirs, start + k * step, step)], sems.at[k]
        )

    @pl.loop(0, steps)
    def _(k):
        here = pl.ds(pl.multiple_of(k * step, step), step)
        at = pl.ds(pl.multiple_of(start + k * step, 64), step)
        for c in tiles(cols):
            factor = jnp.broadcast_to(scale[pl.ds(which, 1), c], (step, TILE))
            grown = far[here, c].astype(f32) + delta(far_low[which, at, :], high[which, :, c])
            out[here, c] = (grown * widened(far_wide, at) * factor).astype(bf16)
        if keep:
            pl.when(k < steps - keep)(copy(k).start)
        else:
            copy(k).start()

    return [copy(k) for k in range(steps - keep)]


def second_kernel(
    keep,
    kept_gate, kept_up, small, far_small, far_gate, high,
    ready_gate, ready_up, column_gate, column_up, far_low, far_wide, scale, out_far, ahead,
    out_gate, out_up, column, sems, far_sems, column_sems,
):
    rows, cols = kept_gate.shape
    rank = high.shape[1]
    me = lax.axis_index("fsdp")
    mine, theirs = me * rows, (1 - me) * rows
    waits = []
    for which, kept, ready, out, column_to in (
        (0, kept_gate, ready_gate, out_gate, column_gate),
        (1, kept_up, ready_up, out_up, column_up),
    ):
        top = jnp.maximum(top_row(small, rank, which), top_row(far_small, rank, which))
        scale[pl.ds(which, 1), :] = 1.0 / top

        def copy(k):
            return pltpu.make_async_copy(
                out.at[pl.ds(pl.multiple_of(k * OWN_ROWS, OWN_ROWS), OWN_ROWS)],
                ready.at[rows_at(mine, k * OWN_ROWS, OWN_ROWS)],
                sems.at[which, k],
            )

        @pl.loop(0, rows // OWN_ROWS)
        def _(k):
            at = pl.ds(pl.multiple_of(k * OWN_ROWS, OWN_ROWS), OWN_ROWS)
            for c in tiles(cols):
                factor = jnp.broadcast_to(scale[pl.ds(which, 1), c], (OWN_ROWS, TILE))
                out[at, c] = (kept[at, c] * factor).astype(bf16)
            copy(k).start()

        waits += [copy(k) for k in range(rows // OWN_ROWS)]
        for k in range(cols // LANES):
            column[which, pl.ds(k, 1), :] = top[:, k * LANES : (k + 1) * LANES]
        waits.append(pltpu.make_async_copy(column.at[which], column_to, column_sems.at[which]))
        waits[-1].start()
    spread_gain(
        lambda k: far_small[pl.ds(2 * rank, 1), pl.ds(k * LANES, LANES)], far_wide
    )
    for w in range(2):
        far_low[w] = far_small[pl.ds(w * rank, rank), :].T.astype(bf16)
    waits += scale_far(
        far_gate, 0, 0, FAR_ROWS, far_low, far_wide, scale, high, out_far, ready_gate, theirs, far_sems, keep
    )
    size = ahead.shape[0]

    @pl.loop(0, size // AHEAD_ROWS)
    def _(k):
        here = pl.ds(pl.multiple_of(k * AHEAD_ROWS, AHEAD_ROWS), AHEAD_ROWS)
        at = pl.ds(pl.multiple_of(rows - size + k * AHEAD_ROWS, 64), AHEAD_ROWS)
        for c in tiles(cols):
            factor = jnp.broadcast_to(scale[pl.ds(1, 1), c], (AHEAD_ROWS, TILE))
            ahead[here, c] = delta(far_low[1, at, :], high[1, :, c]) * widened(far_wide, at) * factor

    for c in waits:
        c.wait()


def far_kernel(
    start, step, behind, keep,
    far_up, far_low, far_wide, scale, high, carried, before_gate, before_up,
    ready_gate, ready_up, *rest,
):
    out, sems = rest[:2]
    rows = far_wide.shape[0]
    theirs = (1 - lax.axis_index("fsdp")) * rows
    which, at, size = behind
    n = carried.shape[0]
    carry = pltpu.make_async_copy(
        carried.at[pl.ds(n - size, size)],
        (ready_gate, ready_up)[which].at[rows_at(theirs, at, size)],
        rest[2],
    )
    carry.start()
    waits = scale_far(
        far_up, 1, start, step, far_low, far_wide, scale, high, out, ready_up, theirs, sems, keep
    )
    carry.wait()
    for c in waits:
        c.wait()


def end_kernel(
    start, behind,
    far_up, far_wide, scale, ahead, carried, before_gate, before_up,
    ready_gate, ready_up, out, sems, carry_sem,
):
    size, cols = far_up.shape
    rows = far_wide.shape[0]
    theirs = (1 - lax.axis_index("fsdp")) * rows
    which, at, behind_size = behind
    n = carried.shape[0]
    carry = pltpu.make_async_copy(
        carried.at[pl.ds(n - behind_size, behind_size)],
        (ready_gate, ready_up)[which].at[rows_at(theirs, at, behind_size)],
        carry_sem,
    )
    carry.start()

    def copy(k):
        here = pl.ds(pl.multiple_of(k * LAST_ROWS, LAST_ROWS), LAST_ROWS)
        return pltpu.make_async_copy(
            out.at[here], ready_up.at[rows_at(theirs, start + k * LAST_ROWS, LAST_ROWS)], sems.at[k]
        )

    @pl.loop(0, size // LAST_ROWS)
    def _(k):
        here = pl.ds(pl.multiple_of(k * LAST_ROWS, LAST_ROWS), LAST_ROWS)
        at = pl.ds(pl.multiple_of(start + k * LAST_ROWS, LAST_ROWS), LAST_ROWS)
        for c in tiles(cols):
            factor = jnp.broadcast_to(scale[pl.ds(1, 1), c], (LAST_ROWS, TILE))
            scaled = far_up[here, c].astype(f32) * widened(far_wide, at) * factor
            out[here, c] = (scaled + ahead[here, c]).astype(bf16)
        copy(k).start()

    carry.wait()
    for k in range(size // LAST_ROWS):
        copy(k).wait()


def paired(train_gate, low_gate, high_gate, train_up, low_up, high_up, norm_gain):
    rows, cols = train_gate.shape
    rank = high_gate.shape[0]
    swap = [(0, 1), (1, 0)]
    other = lambda x: lax.ppermute(x, "fsdp", swap)
    pieces = tuple(rows * part // sum(PARTS) for part in PARTS)
    far_gate = other(train_gate)
    n_small = -(-(2 * rank + 5) // SUBLANES) * SUBLANES
    kept = pltpu.VMEM((rows, cols), f32)
    kept_gate, kept_up, small, high, *ups = pl.pallas_call(
        functools.partial(first_kernel, pieces),
        out_shape=[kept, kept, pltpu.VMEM((n_small, rows), f32), pltpu.VMEM((2, rank, cols), bf16)]
        + [pltpu.VMEM((size, cols), bf16) for size in pieces],
        in_specs=[HBM] * 7,
        out_specs=[VMEM] * (4 + len(pieces)),
        scratch_shapes=[
            pltpu.VMEM((rows, cols), bf16),
            pltpu.VMEM((2, rank, rows), bf16),
            pltpu.VMEM((rows // LANES, LANES), f32),
            pltpu.VMEM((2, rows, rank), bf16),
            pltpu.VMEM((rows, LANES), f32),
            pltpu.VMEM((2, SUBLANES, cols), f32),
            pltpu.SemaphoreType.DMA((GATE_STEPS + sum(UP_STEPS),)),
            pltpu.SemaphoreType.DMA((5,)),
        ],
        compiler_params=pltpu.CompilerParams(vmem_limit_bytes=8 << 20),
        name="own_half",
    )(
        in_hbm(train_gate), in_hbm(low_gate.T), in_hbm(high_gate),
        in_hbm(train_up), in_hbm(low_up.T), in_hbm(high_up),
        in_hbm(norm_gain.reshape(rows // LANES, LANES)),
    )
    far_small = other(small)
    far_ups = [other(up) for up in ups]
    whole = jax.ShapeDtypeStruct((2 * rows, cols), bf16)
    column = jax.ShapeDtypeStruct((cols // LANES, LANES), f32)
    keep = KEEP
    ready_gate, ready_up, column_gate, column_up, far_low, far_wide, scale, carry, ahead = pl.pallas_call(
        functools.partial(second_kernel, keep),
        out_shape=[
            whole, whole, column, column,
            pltpu.VMEM((2, rows, rank), bf16), pltpu.VMEM((rows, LANES), f32), pltpu.VMEM((2, cols), f32),
            pltpu.VMEM((rows, cols), bf16), pltpu.VMEM((pieces[-1], cols), f32),
        ],
        in_specs=[VMEM] * 6,
        out_specs=[HBM] * 4 + [VMEM] * 5,
        scratch_shapes=[
            pltpu.VMEM((rows, cols), bf16),
            pltpu.VMEM((rows, cols), bf16),
            pltpu.VMEM((2, cols // LANES, LANES), f32),
            pltpu.SemaphoreType.DMA((2, rows // OWN_ROWS)),
            pltpu.SemaphoreType.DMA((rows // FAR_ROWS,)),
            pltpu.SemaphoreType.DMA((2,)),
        ],
        compiler_params=pltpu.CompilerParams(vmem_limit_bytes=10 << 20),
        name="own_out",
    )(
        in_vmem(kept_gate), in_vmem(kept_up), in_vmem(small), in_vmem(far_small), in_vmem(far_gate),
        in_vmem(high),
    )
    behind = (0, rows - keep * FAR_ROWS, keep * FAR_ROWS)
    *heads, (start, size) = spans(pieces, rows)
    for (at, part), far_up in zip(heads, far_ups):
        ready_gate, ready_up, carry = pl.pallas_call(
            functools.partial(far_kernel, at, HEAD_ROWS, behind, KEEP_UP),
            out_shape=[whole, whole, pltpu.VMEM((part, cols), bf16)],
            in_specs=[VMEM] * 6 + [HBM, HBM],
            out_specs=[HBM, HBM, VMEM],
            scratch_shapes=[pltpu.SemaphoreType.DMA((part // HEAD_ROWS,)), pltpu.SemaphoreType.DMA],
            input_output_aliases={6: 0, 7: 1},
            compiler_params=pltpu.CompilerParams(vmem_limit_bytes=6 << 20),
        )(
            in_vmem(far_up), in_vmem(far_low), in_vmem(far_wide), in_vmem(scale), in_vmem(high),
            in_vmem(carry), ready_gate, ready_up,
        )
        behind = (1, at + part - KEEP_UP * HEAD_ROWS, KEEP_UP * HEAD_ROWS)
    ready_gate, ready_up = pl.pallas_call(
        functools.partial(end_kernel, start, behind),
        out_shape=[whole, whole],
        in_specs=[VMEM] * 5 + [HBM, HBM],
        out_specs=[HBM, HBM],
        scratch_shapes=[
            pltpu.VMEM((size, cols), bf16),
            pltpu.SemaphoreType.DMA((size // LAST_ROWS,)),
            pltpu.SemaphoreType.DMA,
        ],
        input_output_aliases={5: 0, 6: 1},
        compiler_params=pltpu.CompilerParams(vmem_limit_bytes=6 << 20),
        name="far_up_end",
    )(
        in_vmem(far_ups[-1]), in_vmem(far_wide), in_vmem(scale), in_vmem(ahead), in_vmem(carry),
        ready_gate, ready_up,
    )
    return ready_gate, ready_up, column_gate.reshape(cols), column_up.reshape(cols)


def gathered(train_gate, low_gate, high_gate, train_up, low_up, high_up, norm_gain):
    def gained(train, low, high):
        return (train.astype(f32) + delta(low, high)) * norm_gain[:, None]

    gate, up = gained(train_gate, low_gate, high_gate), gained(train_up, low_up, high_up)
    column_gate, column_up = lax.pmax(
        (jnp.max(jnp.abs(gate), axis=0), jnp.max(jnp.abs(up), axis=0)), "fsdp"
    )
    ready_gate, ready_up = (
        lax.all_gather((full / column).astype(bf16), "fsdp", axis=0, tiled=True)
        for full, column in ((gate, column_gate), (up, column_up))
    )
    return ready_gate, ready_up, column_gate, column_up


def solution(mesh):
    placed = (
        P(("trial", "fsdp"), "cols"),
        P(("trial", "fsdp"), None),
        P("trial", "cols"),
        P(("trial", "fsdp"), "cols"),
        P(("trial", "fsdp"), None),
        P("trial", "cols"),
        P(("trial", "fsdp")),
    )
    pair = mesh.shape["fsdp"] == 2
    return jax.shard_map(
        paired if pair else gathered,
        mesh=mesh,
        in_specs=placed,
        out_specs=(
            P("trial", "cols"),
            P("trial", "cols"),
            P(("trial", "cols")),
            P(("trial", "cols")),
        ),
        check_vma=False,
    )
```

```python
import functools

import jax
import jax.numpy as jnp
from jax import lax
from jax.experimental import pallas as pl
from jax.experimental.pallas import tpu as pltpu
from jax.sharding import PartitionSpec as P


mix_rate = 1.0
LANES = 128
SUBLANES = 8
TILE = 256
GATE_STEPS = 4
UP_STEPS = (2, 2)
IN_FLIGHT = 3
OWN_ROWS = 128
FAR_ROWS = 256
HEAD_ROWS = 320
LAST_ROWS = 128
PARTS = (5, 3)
KEEP = 2
AHEAD_ROWS = 384
KEEP_UP = 1
HBM = pl.BlockSpec(memory_space=pl.ANY)
VMEM = pl.BlockSpec(memory_space=pltpu.VMEM)
f32, bf16 = jnp.float32, jnp.bfloat16


def in_hbm(x):
    return pltpu.with_memory_space_constraint(x, pltpu.HBM)


def in_vmem(x):
    return pltpu.with_memory_space_constraint(x, pltpu.VMEM)


def spread_gain(gain_row, wide_ref):
    for k in range(wide_ref.shape[0] // LANES):
        row = gain_row(k)
        wide_ref[pl.ds(k * LANES, LANES), :] = jnp.broadcast_to(row, (LANES, LANES)).T


def delta(low, high):
    return mix_rate * jnp.dot(low, high, preferred_element_type=f32)


def tiles(cols):
    return [pl.ds(j * TILE, TILE) for j in range(cols // TILE)]


def widened(ref, at):
    return jnp.concatenate([ref[at, :]] * (TILE // LANES), axis=1)


def first_kernel(
    pieces,
    train_gate, low_gate, high_gate, train_up, low_up, high_up, gain,
    kept_gate, kept_up, small, low_in, high, *rest,
):
    ups = rest[: len(pieces)]
    held, gain_in, low, wide, peak, sems, small_sems = rest[len(pieces) :]
    rows, cols = train_gate.shape
    small_copies = [
        pltpu.make_async_copy(src, dst, small_sems.at[n])
        for n, (src, dst) in enumerate(
            (
                (gain, gain_in),
                (low_gate, low_in.at[0]),
                (high_gate, high.at[0]),
                (low_up, low_in.at[1]),
                (high_up, high.at[1]),
            )
        )
    ]
    groups = [(0, 0, rows, rows // GATE_STEPS, train_gate, held, kept_gate)]
    groups += [
        (1, start, size, size // steps, train_up, up, kept_up)
        for up, (start, size), steps in zip(ups, spans(pieces, rows), UP_STEPS)
    ]
    copies = []
    for _, start, size, step, train, dst, _ in groups:
        for at in range(0, size, step):
            n = len(copies)
            copies.append(
                pltpu.make_async_copy(
                    train.at[pl.ds(start + at, step)], dst.at[pl.ds(at, step)], sems.at[n]
                )
            )
    copies[0].start()
    for c in small_copies:
        c.start()
    for c in copies[1:IN_FLIGHT]:
        c.start()
    for c in small_copies:
        c.wait()
    spread_gain(lambda k: gain_in[pl.ds(k, 1), :], wide)
    for which in range(2):
        low[which] = low_in[which].astype(f32).T.astype(bf16)
    for k in range(rows // LANES):
        small[pl.ds(0, 1), pl.ds(k * LANES, LANES)] = gain_in[pl.ds(k, 1), :]
    peak[...] = jnp.zeros_like(peak)
    done = 0
    for which, start, size, step, train, src, kept in groups:
        steps = size // step

        @pl.loop(0, steps)
        def _(k):
            pltpu.make_async_copy(
                train.at[pl.ds(0, step)], src.at[pl.ds(0, step)], sems.at[done + k]
            ).wait()
            for ahead in range(done + IN_FLIGHT, min(done + steps + IN_FLIGHT, len(copies))):
                pl.when(done + k + IN_FLIGHT == ahead)(copies[ahead].start)
            here = pl.ds(pl.multiple_of(k * step, step), step)
            at = pl.ds(pl.multiple_of(start + k * step, 64), step)
            for c in tiles(cols):
                grown = src[here, c].astype(f32) + delta(low[which, at, :], high[which, :, c])
                gained = grown * widened(wide, at)
                kept[at, c] = gained
                top = jnp.max(jnp.abs(gained).reshape(step // SUBLANES, SUBLANES, TILE), axis=0)
                peak[which, :, c] = jnp.maximum(peak[which, :, c], top)

        done += steps
    line = cols // 2
    for which in range(2):
        top = jnp.max(peak[which], axis=0, keepdims=True)
        for half in range(2):
            small[pl.ds(1 + 2 * which + half, 1), :] = top[:, half * line : (half + 1) * line]


def spans(sizes, total):
    start, out = 0, []
    while start < total:
        size = min(sizes[min(len(out), len(sizes) - 1)], total - start)
        out.append((start, size))
        start += size
    return out


def top_row(ref, which):
    base = 1 + 2 * which
    return jnp.concatenate([ref[pl.ds(base, 1), :], ref[pl.ds(base + 1, 1), :]], axis=1)


def rows_at(base, start, size):
    return pl.ds(pl.multiple_of(base + start, 64), size)


def scale_far(far, which, start, step, far_low, far_wide, scale, high, out, target, theirs, sems, keep):
    size, cols = far.shape
    steps = size // step

    def copy(k):
        here = pl.ds(pl.multiple_of(k * step, step), step)
        return pltpu.make_async_copy(
            out.at[here], target.at[rows_at(theirs, start + k * step, step)], sems.at[k]
        )

    @pl.loop(0, steps)
    def _(k):
        here = pl.ds(pl.multiple_of(k * step, step), step)
        at = pl.ds(pl.multiple_of(start + k * step, 64), step)
        for c in tiles(cols):
            factor = jnp.broadcast_to(scale[pl.ds(which, 1), c], (step, TILE))
            grown = far[here, c].astype(f32) + delta(far_low[which, at, :], high[which, :, c])
            out[here, c] = (grown * widened(far_wide, at) * factor).astype(bf16)
        if keep:
            pl.when(k < steps - keep)(copy(k).start)
        else:
            copy(k).start()

    return [copy(k) for k in range(steps - keep)]


def second_kernel(
    keep,
    kept_gate, kept_up, small, far_small, far_lows, far_gate, high,
    ready_gate, ready_up, column_gate, column_up, far_low, far_wide, scale, out_far, ahead,
    out_gate, out_up, column, sems, far_sems, column_sems,
):
    rows, cols = kept_gate.shape
    me = lax.axis_index("fsdp")
    mine, theirs = me * rows, (1 - me) * rows
    waits = []
    for which, kept, ready, out, column_to in (
        (0, kept_gate, ready_gate, out_gate, column_gate),
        (1, kept_up, ready_up, out_up, column_up),
    ):
        top = jnp.maximum(top_row(small, which), top_row(far_small, which))
        scale[pl.ds(which, 1), :] = 1.0 / top

        def copy(k):
            return pltpu.make_async_copy(
                out.at[pl.ds(pl.multiple_of(k * OWN_ROWS, OWN_ROWS), OWN_ROWS)],
                ready.at[rows_at(mine, k * OWN_ROWS, OWN_ROWS)],
                sems.at[which, k],
            )

        @pl.loop(0, rows // OWN_ROWS)
        def _(k):
            at = pl.ds(pl.multiple_of(k * OWN_ROWS, OWN_ROWS), OWN_ROWS)
            for c in tiles(cols):
                factor = jnp.broadcast_to(scale[pl.ds(which, 1), c], (OWN_ROWS, TILE))
                out[at, c] = (kept[at, c] * factor).astype(bf16)
            copy(k).start()

        waits += [copy(k) for k in range(rows // OWN_ROWS)]
        for k in range(cols // LANES):
            column[which, pl.ds(k, 1), :] = top[:, k * LANES : (k + 1) * LANES]
        waits.append(pltpu.make_async_copy(column.at[which], column_to, column_sems.at[which]))
        waits[-1].start()
    spread_gain(
        lambda k: far_small[pl.ds(0, 1), pl.ds(k * LANES, LANES)], far_wide
    )
    for w in range(2):
        far_low[w] = far_lows[w].astype(f32).T.astype(bf16)
    waits += scale_far(
        far_gate, 0, 0, FAR_ROWS, far_low, far_wide, scale, high, out_far, ready_gate, theirs, far_sems, keep
    )
    size = ahead.shape[0]

    @pl.loop(0, size // AHEAD_ROWS)
    def _(k):
        here = pl.ds(pl.multiple_of(k * AHEAD_ROWS, AHEAD_ROWS), AHEAD_ROWS)
        at = pl.ds(pl.multiple_of(rows - size + k * AHEAD_ROWS, 64), AHEAD_ROWS)
        for c in tiles(cols):
            factor = jnp.broadcast_to(scale[pl.ds(1, 1), c], (AHEAD_ROWS, TILE))
            ahead[here, c] = delta(far_low[1, at, :], high[1, :, c]) * widened(far_wide, at) * factor

    for c in waits:
        c.wait()


def far_kernel(
    start, step, behind, keep,
    far_up, far_low, far_wide, scale, high, carried, before_gate, before_up,
    ready_gate, ready_up, *rest,
):
    out, sems = rest[:2]
    rows = far_wide.shape[0]
    theirs = (1 - lax.axis_index("fsdp")) * rows
    which, at, size = behind
    n = carried.shape[0]
    carry = pltpu.make_async_copy(
        carried.at[pl.ds(n - size, size)],
        (ready_gate, ready_up)[which].at[rows_at(theirs, at, size)],
        rest[2],
    )
    carry.start()
    waits = scale_far(
        far_up, 1, start, step, far_low, far_wide, scale, high, out, ready_up, theirs, sems, keep
    )
    carry.wait()
    for c in waits:
        c.wait()


def end_kernel(
    start, behind,
    far_up, far_wide, scale, ahead, carried, before_gate, before_up,
    ready_gate, ready_up, out, sems, carry_sem,
):
    size, cols = far_up.shape
    rows = far_wide.shape[0]
    theirs = (1 - lax.axis_index("fsdp")) * rows
    which, at, behind_size = behind
    n = carried.shape[0]
    carry = pltpu.make_async_copy(
        carried.at[pl.ds(n - behind_size, behind_size)],
        (ready_gate, ready_up)[which].at[rows_at(theirs, at, behind_size)],
        carry_sem,
    )
    carry.start()

    def copy(k):
        here = pl.ds(pl.multiple_of(k * LAST_ROWS, LAST_ROWS), LAST_ROWS)
        return pltpu.make_async_copy(
            out.at[here], ready_up.at[rows_at(theirs, start + k * LAST_ROWS, LAST_ROWS)], sems.at[k]
        )

    @pl.loop(0, size // LAST_ROWS)
    def _(k):
        here = pl.ds(pl.multiple_of(k * LAST_ROWS, LAST_ROWS), LAST_ROWS)
        at = pl.ds(pl.multiple_of(start + k * LAST_ROWS, LAST_ROWS), LAST_ROWS)
        for c in tiles(cols):
            factor = jnp.broadcast_to(scale[pl.ds(1, 1), c], (LAST_ROWS, TILE))
            scaled = far_up[here, c].astype(f32) * widened(far_wide, at) * factor
            out[here, c] = (scaled + ahead[here, c]).astype(bf16)
        copy(k).start()

    carry.wait()
    for k in range(size // LAST_ROWS):
        copy(k).wait()


def paired(train_gate, low_gate, high_gate, train_up, low_up, high_up, norm_gain):
    rows, cols = train_gate.shape
    rank = high_gate.shape[0]
    swap = [(0, 1), (1, 0)]
    other = lambda x: lax.ppermute(x, "fsdp", swap)
    pieces = tuple(rows * part // sum(PARTS) for part in PARTS)
    far_gate = other(train_gate)
    kept = pltpu.VMEM((rows, cols), f32)
    kept_gate, kept_up, small, lows, high, *ups = pl.pallas_call(
        functools.partial(first_kernel, pieces),
        out_shape=[
            kept, kept, pltpu.VMEM((SUBLANES, rows), f32),
            pltpu.VMEM((2, rank, rows), bf16), pltpu.VMEM((2, rank, cols), bf16),
        ]
        + [pltpu.VMEM((size, cols), bf16) for size in pieces],
        in_specs=[HBM] * 7,
        out_specs=[VMEM] * (5 + len(pieces)),
        scratch_shapes=[
            pltpu.VMEM((rows, cols), bf16),
            pltpu.VMEM((rows // LANES, LANES), f32),
            pltpu.VMEM((2, rows, rank), bf16),
            pltpu.VMEM((rows, LANES), f32),
            pltpu.VMEM((2, SUBLANES, cols), f32),
            pltpu.SemaphoreType.DMA((GATE_STEPS + sum(UP_STEPS),)),
            pltpu.SemaphoreType.DMA((5,)),
        ],
        compiler_params=pltpu.CompilerParams(vmem_limit_bytes=8 << 20),
        name="own_half",
    )(
        in_hbm(train_gate), in_hbm(low_gate.T), in_hbm(high_gate),
        in_hbm(train_up), in_hbm(low_up.T), in_hbm(high_up),
        in_hbm(norm_gain.reshape(rows // LANES, LANES)),
    )
    far_small = other(small)
    far_lows = other(lows)
    far_ups = [other(up) for up in ups]
    whole = jax.ShapeDtypeStruct((2 * rows, cols), bf16)
    column = jax.ShapeDtypeStruct((cols // LANES, LANES), f32)
    keep = KEEP
    ready_gate, ready_up, column_gate, column_up, far_low, far_wide, scale, carry, ahead = pl.pallas_call(
        functools.partial(second_kernel, keep),
        out_shape=[
            whole, whole, column, column,
            pltpu.VMEM((2, rows, rank), bf16), pltpu.VMEM((rows, LANES), f32), pltpu.VMEM((2, cols), f32),
            pltpu.VMEM((rows, cols), bf16), pltpu.VMEM((pieces[-1], cols), f32),
        ],
        in_specs=[VMEM] * 7,
        out_specs=[HBM] * 4 + [VMEM] * 5,
        scratch_shapes=[
            pltpu.VMEM((rows, cols), bf16),
            pltpu.VMEM((rows, cols), bf16),
            pltpu.VMEM((2, cols // LANES, LANES), f32),
            pltpu.SemaphoreType.DMA((2, rows // OWN_ROWS)),
            pltpu.SemaphoreType.DMA((rows // FAR_ROWS,)),
            pltpu.SemaphoreType.DMA((2,)),
        ],
        compiler_params=pltpu.CompilerParams(vmem_limit_bytes=10 << 20),
        name="own_out",
    )(
        in_vmem(kept_gate), in_vmem(kept_up), in_vmem(small), in_vmem(far_small), in_vmem(far_lows),
        in_vmem(far_gate),
        in_vmem(high),
    )
    behind = (0, rows - keep * FAR_ROWS, keep * FAR_ROWS)
    *heads, (start, size) = spans(pieces, rows)
    for (at, part), far_up in zip(heads, far_ups):
        ready_gate, ready_up, carry = pl.pallas_call(
            functools.partial(far_kernel, at, HEAD_ROWS, behind, KEEP_UP),
            out_shape=[whole, whole, pltpu.VMEM((part, cols), bf16)],
            in_specs=[VMEM] * 6 + [HBM, HBM],
            out_specs=[HBM, HBM, VMEM],
            scratch_shapes=[pltpu.SemaphoreType.DMA((part // HEAD_ROWS,)), pltpu.SemaphoreType.DMA],
            input_output_aliases={6: 0, 7: 1},
            compiler_params=pltpu.CompilerParams(vmem_limit_bytes=6 << 20),
        )(
            in_vmem(far_up), in_vmem(far_low), in_vmem(far_wide), in_vmem(scale), in_vmem(high),
            in_vmem(carry), ready_gate, ready_up,
        )
        behind = (1, at + part - KEEP_UP * HEAD_ROWS, KEEP_UP * HEAD_ROWS)
    ready_gate, ready_up = pl.pallas_call(
        functools.partial(end_kernel, start, behind),
        out_shape=[whole, whole],
        in_specs=[VMEM] * 5 + [HBM, HBM],
        out_specs=[HBM, HBM],
        scratch_shapes=[
            pltpu.VMEM((size, cols), bf16),
            pltpu.SemaphoreType.DMA((size // LAST_ROWS,)),
            pltpu.SemaphoreType.DMA,
        ],
        input_output_aliases={5: 0, 6: 1},
        compiler_params=pltpu.CompilerParams(vmem_limit_bytes=6 << 20),
        name="far_up_end",
    )(
        in_vmem(far_ups[-1]), in_vmem(far_wide), in_vmem(scale), in_vmem(ahead), in_vmem(carry),
        ready_gate, ready_up,
    )
    return ready_gate, ready_up, column_gate.reshape(cols), column_up.reshape(cols)


def gathered(train_gate, low_gate, high_gate, train_up, low_up, high_up, norm_gain):
    def gained(train, low, high):
        return (train.astype(f32) + delta(low, high)) * norm_gain[:, None]

    gate, up = gained(train_gate, low_gate, high_gate), gained(train_up, low_up, high_up)
    column_gate, column_up = lax.pmax(
        (jnp.max(jnp.abs(gate), axis=0), jnp.max(jnp.abs(up), axis=0)), "fsdp"
    )
    ready_gate, ready_up = (
        lax.all_gather((full / column).astype(bf16), "fsdp", axis=0, tiled=True)
        for full, column in ((gate, column_gate), (up, column_up))
    )
    return ready_gate, ready_up, column_gate, column_up


def solution(mesh):
    placed = (
        P(("trial", "fsdp"), "cols"),
        P(("trial", "fsdp"), None),
        P("trial", "cols"),
        P(("trial", "fsdp"), "cols"),
        P(("trial", "fsdp"), None),
        P("trial", "cols"),
        P(("trial", "fsdp")),
    )
    pair = mesh.shape["fsdp"] == 2
    return jax.shard_map(
        paired if pair else gathered,
        mesh=mesh,
        in_specs=placed,
        out_specs=(
            P("trial", "cols"),
            P("trial", "cols"),
            P(("trial", "cols")),
            P(("trial", "cols")),
        ),
        check_vma=False,
    )
```

```python
import functools

import jax
import jax.numpy as jnp
from jax import lax
from jax.experimental import pallas as pl
from jax.experimental.pallas import tpu as pltpu
from jax.sharding import PartitionSpec as P


mix_rate = 1.0
LANES = 128
SUBLANES = 8
TILE = 256
GATE_STEPS = 4
UP_STEPS = (2, 2)
IN_FLIGHT = 3
OWN_ROWS = 128
FAR_ROWS = 256
HEAD_ROWS = 320
LAST_ROWS = 128
PARTS = (5, 3)
KEEP = 2
AHEAD_ROWS = 384
KEEP_UP = 1
HBM = pl.BlockSpec(memory_space=pl.ANY)
VMEM = pl.BlockSpec(memory_space=pltpu.VMEM)
f32, bf16 = jnp.float32, jnp.bfloat16


def in_hbm(x):
    return pltpu.with_memory_space_constraint(x, pltpu.HBM)


def in_vmem(x):
    return pltpu.with_memory_space_constraint(x, pltpu.VMEM)


def spread_gain(gain_row, wide_ref):
    for k in range(wide_ref.shape[0] // LANES):
        row = gain_row(k)
        wide_ref[pl.ds(k * LANES, LANES), :] = jnp.broadcast_to(row, (LANES, LANES)).T


def delta(low, high):
    return mix_rate * jnp.dot(low, high, preferred_element_type=f32)


def tiles(cols):
    return [pl.ds(j * TILE, TILE) for j in range(cols // TILE)]


def widened(ref, at):
    return jnp.concatenate([ref[at, :]] * (TILE // LANES), axis=1)


def first_kernel(
    pieces,
    train_gate, low_gate, high_gate, train_up, low_up, high_up, gain,
    kept_gate, kept_up, small, low_in, high, *rest,
):
    ups = rest[: len(pieces)]
    held, gain_in, low, wide, peak, sems, small_sems = rest[len(pieces) :]
    rows, cols = train_gate.shape
    small_copies = [
        pltpu.make_async_copy(src, dst, small_sems.at[n])
        for n, (src, dst) in enumerate(
            (
                (gain, gain_in),
                (low_gate, low_in.at[0]),
                (high_gate, high.at[0]),
                (low_up, low_in.at[1]),
                (high_up, high.at[1]),
            )
        )
    ]
    groups = [(0, 0, rows, rows // GATE_STEPS, train_gate, held, kept_gate)]
    groups += [
        (1, start, size, size // steps, train_up, up, kept_up)
        for up, (start, size), steps in zip(ups, spans(pieces, rows), UP_STEPS)
    ]
    copies = []
    for _, start, size, step, train, dst, _ in groups:
        for at in range(0, size, step):
            n = len(copies)
            copies.append(
                pltpu.make_async_copy(
                    train.at[pl.ds(start + at, step)], dst.at[pl.ds(at, step)], sems.at[n]
                )
            )
    copies[0].start()
    for c in small_copies:
        c.start()
    for c in copies[1:IN_FLIGHT]:
        c.start()
    for c in small_copies:
        c.wait()
    spread_gain(lambda k: gain_in[pl.ds(k, 1), :], wide)
    for which in range(2):
        low[which] = low_in[which].astype(f32).T.astype(bf16)
    for k in range(rows // LANES):
        small[pl.ds(4, 1), pl.ds(k * LANES, LANES)] = gain_in[pl.ds(k, 1), :]
    peak[...] = jnp.zeros_like(peak)
    done = 0
    for which, start, size, step, train, src, kept in groups:
        steps = size // step

        @pl.loop(0, steps)
        def _(k):
            pltpu.make_async_copy(
                train.at[pl.ds(0, step)], src.at[pl.ds(0, step)], sems.at[done + k]
            ).wait()
            for ahead in range(done + IN_FLIGHT, min(done + steps + IN_FLIGHT, len(copies))):
                pl.when(done + k + IN_FLIGHT == ahead)(copies[ahead].start)
            here = pl.ds(pl.multiple_of(k * step, step), step)
            at = pl.ds(pl.multiple_of(start + k * step, 64), step)
            for c in tiles(cols):
                grown = src[here, c].astype(f32) + delta(low[which, at, :], high[which, :, c])
                gained = grown * widened(wide, at)
                kept[at, c] = gained
                top = jnp.max(jnp.abs(gained).reshape(step // SUBLANES, SUBLANES, TILE), axis=0)
                peak[which, :, c] = jnp.maximum(peak[which, :, c], top)

        done += steps
    line = cols // 2
    for which in range(2):
        top = jnp.max(peak[which], axis=0, keepdims=True)
        for half in range(2):
            small[pl.ds(2 * which + half, 1), :] = top[:, half * line : (half + 1) * line]


def spans(sizes, total):
    start, out = 0, []
    while start < total:
        size = min(sizes[min(len(out), len(sizes) - 1)], total - start)
        out.append((start, size))
        start += size
    return out


def factor_of(scale, which, c, size):
    half = scale.shape[1]
    row = pl.ds(2 * which + c.start // half, 1)
    return jnp.broadcast_to(scale[row, pl.ds(c.start % half, TILE)], (size, TILE))


def rows_at(base, start, size):
    return pl.ds(pl.multiple_of(base + start, 64), size)


def scale_far(far, which, start, step, far_low, far_wide, scale, high, out, target, theirs, sems, keep):
    size, cols = far.shape
    steps = size // step

    def copy(k):
        here = pl.ds(pl.multiple_of(k * step, step), step)
        return pltpu.make_async_copy(
            out.at[here], target.at[rows_at(theirs, start + k * step, step)], sems.at[k]
        )

    @pl.loop(0, steps)
    def _(k):
        here = pl.ds(pl.multiple_of(k * step, step), step)
        at = pl.ds(pl.multiple_of(start + k * step, 64), step)
        for c in tiles(cols):
            factor = factor_of(scale, which, c, step)
            grown = far[here, c].astype(f32) + delta(far_low[which, at, :], high[which, :, c])
            out[here, c] = (grown * widened(far_wide, at) * factor).astype(bf16)
        if keep:
            pl.when(k < steps - keep)(copy(k).start)
        else:
            copy(k).start()

    return [copy(k) for k in range(steps - keep)]


def second_kernel(
    keep,
    kept_gate, kept_up, small, far_small, far_lows, far_gate, high,
    ready_gate, ready_up, column_gate, column_up, far_low, far_wide, scale, out_far, ahead,
    out_gate, out_up, column, sems, far_sems, column_sems,
):
    rows, cols = kept_gate.shape
    me = lax.axis_index("fsdp")
    mine, theirs = me * rows, (1 - me) * rows
    line = cols // 2
    waits = []
    tops = jnp.maximum(small[pl.ds(0, 4), :], far_small[pl.ds(0, 4), :])
    scale[...] = 1.0 / tops
    for which, kept, ready, out, column_to in (
        (0, kept_gate, ready_gate, out_gate, column_gate),
        (1, kept_up, ready_up, out_up, column_up),
    ):
        def copy(k):
            return pltpu.make_async_copy(
                out.at[pl.ds(pl.multiple_of(k * OWN_ROWS, OWN_ROWS), OWN_ROWS)],
                ready.at[rows_at(mine, k * OWN_ROWS, OWN_ROWS)],
                sems.at[which, k],
            )

        @pl.loop(0, rows // OWN_ROWS)
        def _(k):
            at = pl.ds(pl.multiple_of(k * OWN_ROWS, OWN_ROWS), OWN_ROWS)
            for c in tiles(cols):
                factor = factor_of(scale, which, c, OWN_ROWS)
                out[at, c] = (kept[at, c] * factor).astype(bf16)
            copy(k).start()

        waits += [copy(k) for k in range(rows // OWN_ROWS)]
        for k in range(cols // LANES):
            row, at = 2 * which + k * LANES // line, k * LANES % line
            column[which, pl.ds(k, 1), :] = tops[row : row + 1, at : at + LANES]
        waits.append(pltpu.make_async_copy(column.at[which], column_to, column_sems.at[which]))
        waits[-1].start()
    spread_gain(
        lambda k: far_small[pl.ds(4, 1), pl.ds(k * LANES, LANES)], far_wide
    )
    for w in range(2):
        far_low[w] = far_lows[w].astype(f32).T.astype(bf16)
    waits += scale_far(
        far_gate, 0, 0, FAR_ROWS, far_low, far_wide, scale, high, out_far, ready_gate, theirs, far_sems, keep
    )
    size = ahead.shape[0]

    @pl.loop(0, size // AHEAD_ROWS)
    def _(k):
        here = pl.ds(pl.multiple_of(k * AHEAD_ROWS, AHEAD_ROWS), AHEAD_ROWS)
        at = pl.ds(pl.multiple_of(rows - size + k * AHEAD_ROWS, 64), AHEAD_ROWS)
        for c in tiles(cols):
            factor = factor_of(scale, 1, c, AHEAD_ROWS)
            ahead[here, c] = delta(far_low[1, at, :], high[1, :, c]) * widened(far_wide, at) * factor

    for c in waits:
        c.wait()


def far_kernel(
    start, step, behind, keep,
    far_up, far_low, far_wide, scale, high, carried, before_gate, before_up,
    ready_gate, ready_up, *rest,
):
    out, sems = rest[:2]
    rows = far_wide.shape[0]
    theirs = (1 - lax.axis_index("fsdp")) * rows
    which, at, size = behind
    n = carried.shape[0]
    carry = pltpu.make_async_copy(
        carried.at[pl.ds(n - size, size)],
        (ready_gate, ready_up)[which].at[rows_at(theirs, at, size)],
        rest[2],
    )
    carry.start()
    waits = scale_far(
        far_up, 1, start, step, far_low, far_wide, scale, high, out, ready_up, theirs, sems, keep
    )
    carry.wait()
    for c in waits:
        c.wait()


def end_kernel(
    start, behind,
    far_up, far_wide, scale, ahead, carried, before_gate, before_up,
    ready_gate, ready_up, out, sems, carry_sem,
):
    size, cols = far_up.shape
    rows = far_wide.shape[0]
    theirs = (1 - lax.axis_index("fsdp")) * rows
    which, at, behind_size = behind
    n = carried.shape[0]
    carry = pltpu.make_async_copy(
        carried.at[pl.ds(n - behind_size, behind_size)],
        (ready_gate, ready_up)[which].at[rows_at(theirs, at, behind_size)],
        carry_sem,
    )
    carry.start()

    def copy(k):
        here = pl.ds(pl.multiple_of(k * LAST_ROWS, LAST_ROWS), LAST_ROWS)
        return pltpu.make_async_copy(
            out.at[here], ready_up.at[rows_at(theirs, start + k * LAST_ROWS, LAST_ROWS)], sems.at[k]
        )

    @pl.loop(0, size // LAST_ROWS)
    def _(k):
        here = pl.ds(pl.multiple_of(k * LAST_ROWS, LAST_ROWS), LAST_ROWS)
        at = pl.ds(pl.multiple_of(start + k * LAST_ROWS, LAST_ROWS), LAST_ROWS)
        for c in tiles(cols):
            factor = factor_of(scale, 1, c, LAST_ROWS)
            scaled = far_up[here, c].astype(f32) * widened(far_wide, at) * factor
            out[here, c] = (scaled + ahead[here, c]).astype(bf16)
        copy(k).start()

    carry.wait()
    for k in range(size // LAST_ROWS):
        copy(k).wait()


def paired(train_gate, low_gate, high_gate, train_up, low_up, high_up, norm_gain):
    rows, cols = train_gate.shape
    rank = high_gate.shape[0]
    swap = [(0, 1), (1, 0)]
    other = lambda x: lax.ppermute(x, "fsdp", swap)
    pieces = tuple(rows * part // sum(PARTS) for part in PARTS)
    far_gate = other(train_gate)
    kept = pltpu.VMEM((rows, cols), f32)
    kept_gate, kept_up, small, lows, high, *ups = pl.pallas_call(
        functools.partial(first_kernel, pieces),
        out_shape=[
            kept, kept, pltpu.VMEM((SUBLANES, rows), f32),
            pltpu.VMEM((2, rank, rows), bf16), pltpu.VMEM((2, rank, cols), bf16),
        ]
        + [pltpu.VMEM((size, cols), bf16) for size in pieces],
        in_specs=[HBM] * 7,
        out_specs=[VMEM] * (5 + len(pieces)),
        scratch_shapes=[
            pltpu.VMEM((rows, cols), bf16),
            pltpu.VMEM((rows // LANES, LANES), f32),
            pltpu.VMEM((2, rows, rank), bf16),
            pltpu.VMEM((rows, LANES), f32),
            pltpu.VMEM((2, SUBLANES, cols), f32),
            pltpu.SemaphoreType.DMA((GATE_STEPS + sum(UP_STEPS),)),
            pltpu.SemaphoreType.DMA((5,)),
        ],
        compiler_params=pltpu.CompilerParams(vmem_limit_bytes=8 << 20),
        name="own_half",
    )(
        in_hbm(train_gate), in_hbm(low_gate.T), in_hbm(high_gate),
        in_hbm(train_up), in_hbm(low_up.T), in_hbm(high_up),
        in_hbm(norm_gain.reshape(rows // LANES, LANES)),
    )
    far_small = other(small)
    far_lows = other(lows)
    far_ups = [other(up) for up in ups]
    whole = jax.ShapeDtypeStruct((2 * rows, cols), bf16)
    column = jax.ShapeDtypeStruct((cols // LANES, LANES), f32)
    keep = KEEP
    ready_gate, ready_up, column_gate, column_up, far_low, far_wide, scale, carry, ahead = pl.pallas_call(
        functools.partial(second_kernel, keep),
        out_shape=[
            whole, whole, column, column,
            pltpu.VMEM((2, rows, rank), bf16), pltpu.VMEM((rows, LANES), f32), pltpu.VMEM((4, cols // 2), f32),
            pltpu.VMEM((rows, cols), bf16), pltpu.VMEM((pieces[-1], cols), f32),
        ],
        in_specs=[VMEM] * 7,
        out_specs=[HBM] * 4 + [VMEM] * 5,
        scratch_shapes=[
            pltpu.VMEM((rows, cols), bf16),
            pltpu.VMEM((rows, cols), bf16),
            pltpu.VMEM((2, cols // LANES, LANES), f32),
            pltpu.SemaphoreType.DMA((2, rows // OWN_ROWS)),
            pltpu.SemaphoreType.DMA((rows // FAR_ROWS,)),
            pltpu.SemaphoreType.DMA((2,)),
        ],
        compiler_params=pltpu.CompilerParams(vmem_limit_bytes=10 << 20),
        name="own_out",
    )(
        in_vmem(kept_gate), in_vmem(kept_up), in_vmem(small), in_vmem(far_small), in_vmem(far_lows),
        in_vmem(far_gate),
        in_vmem(high),
    )
    behind = (0, rows - keep * FAR_ROWS, keep * FAR_ROWS)
    *heads, (start, size) = spans(pieces, rows)
    for (at, part), far_up in zip(heads, far_ups):
        ready_gate, ready_up, carry = pl.pallas_call(
            functools.partial(far_kernel, at, HEAD_ROWS, behind, KEEP_UP),
            out_shape=[whole, whole, pltpu.VMEM((part, cols), bf16)],
            in_specs=[VMEM] * 6 + [HBM, HBM],
            out_specs=[HBM, HBM, VMEM],
            scratch_shapes=[pltpu.SemaphoreType.DMA((part // HEAD_ROWS,)), pltpu.SemaphoreType.DMA],
            input_output_aliases={6: 0, 7: 1},
            compiler_params=pltpu.CompilerParams(vmem_limit_bytes=6 << 20),
        )(
            in_vmem(far_up), in_vmem(far_low), in_vmem(far_wide), in_vmem(scale), in_vmem(high),
            in_vmem(carry), ready_gate, ready_up,
        )
        behind = (1, at + part - KEEP_UP * HEAD_ROWS, KEEP_UP * HEAD_ROWS)
    ready_gate, ready_up = pl.pallas_call(
        functools.partial(end_kernel, start, behind),
        out_shape=[whole, whole],
        in_specs=[VMEM] * 5 + [HBM, HBM],
        out_specs=[HBM, HBM],
        scratch_shapes=[
            pltpu.VMEM((size, cols), bf16),
            pltpu.SemaphoreType.DMA((size // LAST_ROWS,)),
            pltpu.SemaphoreType.DMA,
        ],
        input_output_aliases={5: 0, 6: 1},
        compiler_params=pltpu.CompilerParams(vmem_limit_bytes=6 << 20),
        name="far_up_end",
    )(
        in_vmem(far_ups[-1]), in_vmem(far_wide), in_vmem(scale), in_vmem(ahead), in_vmem(carry),
        ready_gate, ready_up,
    )
    return ready_gate, ready_up, column_gate.reshape(cols), column_up.reshape(cols)


def gathered(train_gate, low_gate, high_gate, train_up, low_up, high_up, norm_gain):
    def gained(train, low, high):
        return (train.astype(f32) + delta(low, high)) * norm_gain[:, None]

    gate, up = gained(train_gate, low_gate, high_gate), gained(train_up, low_up, high_up)
    column_gate, column_up = lax.pmax(
        (jnp.max(jnp.abs(gate), axis=0), jnp.max(jnp.abs(up), axis=0)), "fsdp"
    )
    ready_gate, ready_up = (
        lax.all_gather((full / column).astype(bf16), "fsdp", axis=0, tiled=True)
        for full, column in ((gate, column_gate), (up, column_up))
    )
    return ready_gate, ready_up, column_gate, column_up


def solution(mesh):
    placed = (
        P(("trial", "fsdp"), "cols"),
        P(("trial", "fsdp"), None),
        P("trial", "cols"),
        P(("trial", "fsdp"), "cols"),
        P(("trial", "fsdp"), None),
        P("trial", "cols"),
        P(("trial", "fsdp")),
    )
    pair = mesh.shape["fsdp"] == 2
    return jax.shard_map(
        paired if pair else gathered,
        mesh=mesh,
        in_specs=placed,
        out_specs=(
            P("trial", "cols"),
            P("trial", "cols"),
            P(("trial", "cols")),
            P(("trial", "cols")),
        ),
        check_vma=False,
    )
```
